64 devices in a mesh: dp: 4 (over x, y), cp: 16 (over z, core).
Axes of the slice: x: 2, y: 2, z: 8, core: 2. Of those that a mesh axis runs over, the one named last changes fastest.
The devices are a block of a 4x4x8 slice.
Arguments:
- x_in: bfloat16 [8192, 1536], P(('dp', 'cp')), parts along dimension 0
- cache_k1: bfloat16 [65536, 2, 128], P(('dp', 'cp')), parts along dimension 0
- cache_v1: bfloat16 [65536, 2, 128], P(('dp', 'cp')), parts along dimension 0
- w_q1: bfloat16 [1536, 1536], replicated
- b_q1: bfloat16 [1536], replicated
- w_k1: bfloat16 [1536, 256], replicated
- b_k1: bfloat16 [256], replicated
- w_v1: bfloat16 [1536, 256], replicated
- w_o1: bfloat16 [1536, 1536], replicated
- w_gate: bfloat16 [1536, 8960], replicated
- w_up: bfloat16 [1536, 8960], replicated
- w_down: bfloat16 [8960, 1536], replicated
- cache_k2: bfloat16 [65536, 2, 128], P(('dp', 'cp')), parts along dimension 0
- cache_v2: bfloat16 [65536, 2, 128], P(('dp', 'cp')), parts along dimension 0
- w_q2: bfloat16 [1536, 1536], replicated
- b_q2: bfloat16 [1536], replicated
- w_k2: bfloat16 [1536, 256], replicated
- b_k2: bfloat16 [256], replicated
- w_v2: bfloat16 [1536, 256], replicated
- w_o2: bfloat16 [1536, 1536], replicated
Outputs:
- output 1: bfloat16 [8192, 1536], P(('dp', 'cp')), parts along dimension 0
- output 2: bfloat16 [8192, 1536], P(('dp', 'cp')), parts along dimension 0
- output 3: bfloat16 [8192, 2, 128], P(('dp', 'cp')), parts along dimension 0
- output 4: bfloat16 [8192, 2, 128], P(('dp', 'cp')), parts along dimension 0
- output 5: bfloat16 [8192, 2, 128], P(('dp', 'cp')), parts along dimension 0
- output 6: bfloat16 [8192, 2, 128], P(('dp', 'cp')), parts along dimension 0
There are 4 independent parts. The reference program is written for one: setup_inputs(seed, part) draws one part's arguments, and reference() takes and returns one part's arrays. A program takes and returns all parts, laid end to end along the dimension named above; an argument that names none is the same for every part.
All inputs are finite; a program needn't handle non-finite values.
Results may differ from the reference program's by a relative error of at most 0.0143816.
Values are sent between devices in bfloat16 or wider.
A program may use at most 768 MiB of HBM per device.

```python
import math
import jax
import jax.numpy as jnp
from jax import lax

D_MODEL = 1536
HEADS = 12
KV_HEADS = 2
HEAD = 128
FF = 8960
CHUNK = 2048
CACHE = 16384
SHARDS = 16
QBLK = 128

GROUP = HEADS // KV_HEADS
SHARD_LEN = CACHE // SHARDS


def draw_matrix(key, rows, cols):
    return (jax.random.normal(key, (rows, cols), jnp.float32) * rows ** -0.5).astype(jnp.bfloat16)


def draw_cache(key_k, key_s, key_v, key_m):
    shard_scale = jax.random.uniform(key_s, (SHARDS, 1, 1, 1), jnp.float32, 0.6, 1.6)
    cache_keys = jax.random.normal(key_k, (SHARDS, SHARD_LEN, KV_HEADS, HEAD), jnp.float32) * shard_scale
    shard_mean = jax.random.normal(key_m, (SHARDS, 1, KV_HEADS, HEAD), jnp.float32)
    cache_vals = 0.5 * jax.random.normal(key_v, (SHARDS, SHARD_LEN, KV_HEADS, HEAD), jnp.float32) + shard_mean
    return (cache_keys.reshape(CACHE, KV_HEADS, HEAD).astype(jnp.bfloat16),
            cache_vals.reshape(CACHE, KV_HEADS, HEAD).astype(jnp.bfloat16))


def draw_bias(key_dir, key_q, key_k):
    half_dim = HEAD // 2
    lane_idx = jnp.arange(HEAD) % half_dim
    low_mask = (lane_idx >= (7 * half_dim) // 8).astype(jnp.float32)
    raw_dir = jax.random.normal(key_dir, (KV_HEADS, HEAD), jnp.float32) * low_mask
    unit_dir = raw_dir / jnp.sqrt(jnp.sum(raw_dir * raw_dir, axis=-1, keepdims=True))
    mean_score = max(math.log(CACHE / CHUNK) + 0.5, 0.5)
    bias_amp = math.sqrt(mean_score * math.sqrt(HEAD))
    jitter_q = jax.random.uniform(key_q, (HEADS, 1), jnp.float32, 0.9, 1.1)
    jitter_k = jax.random.uniform(key_k, (KV_HEADS, 1), jnp.float32, 0.9, 1.1)
    bias_q = bias_amp * jnp.repeat(unit_dir, GROUP, axis=0) * jitter_q
    bias_k = bias_amp * unit_dir * jitter_k
    return (bias_q.reshape(HEADS * HEAD).astype(jnp.bfloat16),
            bias_k.reshape(KV_HEADS * HEAD).astype(jnp.bfloat16))


def setup_inputs(seed: int = 0, part: int = 0) -> dict:
    shared_root, part_root = jax.random.split(jax.random.key(seed))
    part_keys = jax.random.split(jax.random.fold_in(part_root, part), 9)
    weight_keys = jax.random.split(shared_root, 17)
    x_in = jax.random.normal(part_keys[0], (CHUNK, D_MODEL), jnp.float32).astype(jnp.bfloat16)
    cache_k1, cache_v1 = draw_cache(part_keys[1], part_keys[2], part_keys[3], part_keys[4])
    cache_k2, cache_v2 = draw_cache(part_keys[5], part_keys[6], part_keys[7], part_keys[8])
    b_q1, b_k1 = draw_bias(weight_keys[0], weight_keys[1], weight_keys[2])
    b_q2, b_k2 = draw_bias(weight_keys[3], weight_keys[4], weight_keys[5])
    return {
        'x_in': x_in,
        'cache_k1': cache_k1,
        'cache_v1': cache_v1,
        'w_q1': draw_matrix(weight_keys[6], D_MODEL, HEADS * HEAD),
        'b_q1': b_q1,
        'w_k1': draw_matrix(weight_keys[7], D_MODEL, KV_HEADS * HEAD),
        'b_k1': b_k1,
        'w_v1': draw_matrix(weight_keys[8], D_MODEL, KV_HEADS * HEAD),
        'w_o1': draw_matrix(weight_keys[9], HEADS * HEAD, D_MODEL),
        'w_gate': draw_matrix(weight_keys[10], D_MODEL, FF),
        'w_up': draw_matrix(weight_keys[11], D_MODEL, FF),
        'w_down': draw_matrix(weight_keys[12], FF, D_MODEL),
        'cache_k2': cache_k2,
        'cache_v2': cache_v2,
        'w_q2': draw_matrix(weight_keys[13], D_MODEL, HEADS * HEAD),
        'b_q2': b_q2,
        'w_k2': draw_matrix(weight_keys[14], D_MODEL, KV_HEADS * HEAD),
        'b_k2': b_k2,
        'w_v2': draw_matrix(weight_keys[15], D_MODEL, KV_HEADS * HEAD),
        'w_o2': draw_matrix(weight_keys[16], HEADS * HEAD, D_MODEL),
    }


def rms_norm(vals):
    wide = vals.astype(jnp.float32)
    return (wide * lax.rsqrt(jnp.mean(wide * wide, axis=-1, keepdims=True) + 1e-5)).astype(jnp.bfloat16)


def rope_tables(positions):
    half_dim = HEAD // 2
    inv_freq = 1.0 / (500000.0 ** (jnp.arange(half_dim, dtype=jnp.float32) * (2.0 / HEAD)))
    angles = positions.astype(jnp.float32)[:, None] * inv_freq[None, :]
    return jnp.cos(angles)[:, None, :], jnp.sin(angles)[:, None, :]


def apply_rope(vals, cos_t, sin_t):
    half_dim = HEAD // 2
    first = vals[..., :half_dim]
    second = vals[..., half_dim:]
    return jnp.concatenate([first * cos_t - second * sin_t, second * cos_t + first * sin_t], axis=-1)


def attention_layer(layer_in, cache_k, cache_v, w_q, b_q, w_k, b_k, w_v, w_o):
    cos_t, sin_t = rope_tables(CACHE + jnp.arange(CHUNK))
    q_pre = (jnp.dot(layer_in, w_q, preferred_element_type=jnp.float32) + b_q.astype(jnp.float32)).astype(jnp.bfloat16)
    k_pre = (jnp.dot(layer_in, w_k, preferred_element_type=jnp.float32) + b_k.astype(jnp.float32)).astype(jnp.bfloat16)
    v_new = jnp.dot(layer_in, w_v, preferred_element_type=jnp.float32).astype(jnp.bfloat16).reshape(CHUNK, KV_HEADS, HEAD)
    q_rot = apply_rope(q_pre.reshape(CHUNK, HEADS, HEAD).astype(jnp.float32), cos_t, sin_t).astype(jnp.bfloat16)
    k_new = apply_rope(k_pre.reshape(CHUNK, KV_HEADS, HEAD).astype(jnp.float32), cos_t, sin_t).astype(jnp.bfloat16)
    keys_all = jnp.concatenate([cache_k, k_new], axis=0).astype(jnp.float32)
    vals_all = jnp.concatenate([cache_v, v_new], axis=0).astype(jnp.float32)
    key_pos = jnp.arange(CACHE + CHUNK)
    scale = HEAD ** -0.5
    q_blocks = q_rot.reshape(CHUNK // QBLK, QBLK, KV_HEADS, GROUP, HEAD)
    starts = jnp.arange(CHUNK // QBLK) * QBLK

    def one_block(blk_in):
        q_blk, start = blk_in
        scores = jnp.einsum('tkgd,skd->tkgs', q_blk.astype(jnp.float32), keys_all) * scale
        q_pos = CACHE + start + jnp.arange(QBLK)
        visible = key_pos[None, :] <= q_pos[:, None]
        scores = jnp.where(visible[:, None, None, :], scores, -jnp.inf)
        peak = jnp.max(scores, axis=-1, keepdims=True)
        prob_w = jnp.exp(scores - peak)
        total = jnp.sum(prob_w, axis=-1, keepdims=True)
        summed = jnp.einsum('tkgs,skd->tkgd', prob_w.astype(jnp.bfloat16).astype(jnp.float32), vals_all)
        return summed / total

    o_all = lax.map(one_block, (q_blocks, starts))
    o_half = o_all.reshape(CHUNK, HEADS * HEAD).astype(jnp.bfloat16)
    y_out = jnp.dot(o_half, w_o, preferred_element_type=jnp.float32).astype(jnp.bfloat16)
    return y_out, k_new, v_new


def reference(x_in, cache_k1, cache_v1, w_q1, b_q1, w_k1, b_k1, w_v1, w_o1, w_gate, w_up, w_down, cache_k2, cache_v2, w_q2, b_q2, w_k2, b_k2, w_v2, w_o2):
    y_one, k_one, v_one = attention_layer(x_in, cache_k1, cache_v1, w_q1, b_q1, w_k1, b_k1, w_v1, w_o1)
    resid_h = (x_in.astype(jnp.float32) + y_one.astype(jnp.float32)).astype(jnp.bfloat16)
    normed = rms_norm(resid_h)
    gate_act = jnp.dot(normed, w_gate, preferred_element_type=jnp.float32).astype(jnp.bfloat16)
    up_proj = jnp.dot(normed, w_up, preferred_element_type=jnp.float32).astype(jnp.bfloat16)
    mixed = (jax.nn.silu(gate_act.astype(jnp.float32)) * up_proj.astype(jnp.float32)).astype(jnp.bfloat16)
    hidden = (resid_h.astype(jnp.float32) + jnp.dot(mixed, w_down, preferred_element_type=jnp.float32)).astype(jnp.bfloat16)
    y_two, k_two, v_two = attention_layer(rms_norm(hidden), cache_k2, cache_v2, w_q2, b_q2, w_k2, b_k2, w_v2, w_o2)
    return (hidden, y_two, k_one, v_one, k_two, v_two)
```

```python
import functools

import jax
import jax.numpy as jnp
import numpy as np
from jax import lax
from jax.experimental import pallas as pl
from jax.experimental.pallas import tpu as pltpu
from jax.sharding import PartitionSpec as P

ROPE_THETA = 500000.0
NORM_EPS = 1e-5
LOG2E = 1.4426950408889634
BF16 = jnp.bfloat16
F32 = jnp.float32
FF_TILE = 640
W_SLOTS = 3


def rms_norm(wide):
    return (wide * lax.rsqrt(jnp.mean(wide * wide, axis=-1, keepdims=True) + NORM_EPS)).astype(BF16)


def block_kernel(n, x_ref, kc1, vc1, kc2, vc2, wq1, wk1, wv1, wo1, wg, wu, wd, wq2, wk2, wv2, wo2, bias_ref, local_rot, base_rot,
                 g_out, y_out, app_out,
                 kv, nkv, raw, snd, wide, sbuf, cos_ref, sin_ref, knew, vnew, app_in, app_buf,
                 xb, hb, qb, acc, m_s, l_s, ob, gacc, grecv, ybuf, wqkv, wob, w13, w2b,
                 ring_s, ring_r, new_s, new_r, d2d_s, d2d_r, loc, wsem):
    nz = n // 2
    far = nz // 2
    n_arr = 4 * (far - 1) + 2
    n_new = 2 * (far - 1) + 1
    cp = lax.axis_index("cp")
    c = lax.rem(cp, 2)
    z = lax.div(cp, 2)
    partner = cp + 1 - 2 * c
    tok = x_ref.shape[0]
    heads_dev = qb.shape[0]
    hd = qb.shape[1]
    pair = 2 * tok
    cache_dev = kv.shape[4]
    n_steps = n_arr + 2
    half = heads_dev * hd
    ff_half = wg.shape[1] // 2
    tiles = ff_half // FF_TILE
    cache = (kc1, vc1), (kc2, vc2)
    wqkv_src = (wq1, wk1, wv1), (wq2, wk2, wv2)
    wo_src = (wo1, wo2)
    score_mul = hd ** -0.5 * LOG2E

    def toward(direction):
        return {"cp": lax.rem(cp + n + 2 - 4 * direction, n)}

    barrier = pltpu.get_barrier_semaphore()
    for other in (partner, lax.rem(cp + 2, n), lax.rem(cp + n - 2, n)):
        pl.semaphore_signal(barrier, inc=1, device_id={"cp": other})
    pl.semaphore_wait(barrier, 3)

    def load_cache(layer, j):
        return pltpu.make_async_copy(cache[layer][j], raw.at[layer, j], loc.at[1 + 2 * layer + j])

    def swap_cache(layer):
        return pltpu.make_async_remote_copy(snd.at[layer], kv.at[layer, z, c], d2d_s.at[1 + layer], d2d_r.at[1 + layer],
                                            device_id={"cp": partner})

    def split_cache(layer):
        for j in range(2):
            def one_block(b, carry):
                wide[...] = raw[layer, j, pl.ds(pl.multiple_of(b * 2 * hd, 2 * hd), 2 * hd)].astype(F32)
                first = wide[pl.ds(0, hd, stride=2)]
                second = wide[pl.ds(1, hd, stride=2)]
                mine = jnp.where(c == 0, first, second)
                theirs = jnp.where(c == 0, second, first)
                if j == 1:
                    mine, theirs = mine.T, theirs.T
                rows = pl.ds(pl.multiple_of(b * hd, hd), hd)
                kv[layer, z, c, j, rows] = mine.astype(BF16)
                snd[layer, j, rows] = theirs.astype(BF16)
                return carry
            lax.fori_loop(0, cache_dev // hd, one_block, 0)

    own_rows = pl.ds(pl.multiple_of(c * tok, tok), tok)
    other_rows = pl.ds(pl.multiple_of((1 - c) * tok, tok), tok)
    load_x = pltpu.make_async_copy(x_ref, xb.at[own_rows], loc.at[0])
    swap_x = pltpu.make_async_remote_copy(x_ref, xb.at[own_rows], d2d_s.at[0], d2d_r.at[0], device_id={"cp": partner})

    def load_wqkv(layer):
        w_q, w_k, w_v = wqkv_src[layer]
        return (pltpu.make_async_copy(w_q.at[:, pl.ds(pl.multiple_of(c * half, hd), half)], wqkv.at[:, pl.ds(0, half)], loc.at[5]),
                pltpu.make_async_copy(w_k.at[:, pl.ds(pl.multiple_of(c * hd, hd), hd)], wqkv.at[:, pl.ds(half, hd)], loc.at[6]),
                pltpu.make_async_copy(w_v.at[:, pl.ds(pl.multiple_of(c * hd, hd), hd)], wqkv.at[:, pl.ds(half + hd, hd)], loc.at[7]))

    def load_wo(layer):
        return pltpu.make_async_copy(wo_src[layer], wob, loc.at[8])

    def load_ff(tile, slot):
        cols = pl.ds(pl.multiple_of(c * ff_half + tile * FF_TILE, 128), FF_TILE)
        return (pltpu.make_async_copy(wg.at[:, cols], w13.at[slot, :, pl.ds(0, FF_TILE)], wsem.at[slot, 0]),
                pltpu.make_async_copy(wu.at[:, cols], w13.at[slot, :, pl.ds(FF_TILE, FF_TILE)], wsem.at[slot, 1]),
                pltpu.make_async_copy(wd.at[cols], w2b.at[slot], wsem.at[slot, 2]))

    for j in range(2):
        load_cache(0, j).start()
    load_x.start()
    swap_x.start()
    for cpy in load_wqkv(0):
        cpy.start()

    def piece_of(t):
        dist = lax.div(t, 4) + 1
        r = lax.rem(t, 4)
        direction = lax.rem(t, 2)
        order = lax.div(r, 2) + lax.rem(r, 2) * lax.div(dist, far)
        src = lax.rem(z + nz + dist * (2 * direction - 1), nz)
        return src, lax.rem(c + order, 2), direction

    def ring_copy(layer, src, piece, t, direction):
        return pltpu.make_async_remote_copy(kv.at[layer, src, piece], kv.at[layer, src, piece],
                                            ring_s.at[layer, t], ring_r.at[layer, t], device_id=toward(direction))

    def send_own(layer, order):
        for direction in range(2):
            ring_copy(layer, z, lax.rem(c + order, 2), 2 * order + direction, direction).start()

    def arrive(layer, t):
        src, piece, direction = piece_of(t)
        ring_copy(layer, src, piece, t, direction).wait_recv()
        last = 4 * (far - 1)

        @pl.when((t < last - 4) | (t == last - 4) | (t == last - 1))
        def _():
            ring_copy(layer, src, piece, t + 4 - 2 * lax.div(t, last - 1), direction).start()

    def new_piece(u):
        dist = lax.div(u, 2) + 1
        direction = lax.rem(u, 2)
        src_raw = z + dist * (2 * direction - 1)
        return lax.rem(src_raw + nz, nz), direction

    def new_copy(layer, src, u, direction):
        return pltpu.make_async_remote_copy(nkv.at[layer, src], nkv.at[layer, src],
                                            new_s.at[layer, u], new_r.at[layer, u], device_id=toward(direction))

    def attend(k_view, v_view, causal):
        keys = k_view.shape[0]
        kb = min(256, keys)
        blocks = keys // kb

        def scores(h):
            top = None
            for b in range(blocks):
                s = jnp.dot(k_view[b * kb:(b + 1) * kb], qb[h], preferred_element_type=F32)
                if causal:
                    key = lax.broadcasted_iota(jnp.int32, s.shape, 0) + b * kb
                    query = lax.broadcasted_iota(jnp.int32, s.shape, 1)
                    s = jnp.where(key <= query, s, -jnp.inf)
                sbuf[h % 2, b * kb:(b + 1) * kb] = s
                part = jnp.max(s.reshape(kb // 8, 8, pair), axis=0)
                top = part if top is None else jnp.maximum(top, part)
            return top

        top = scores(0)
        for h in range(heads_dev):
            top_next = scores(h + 1) if h + 1 < heads_dev else None
            m_old = m_s[h]
            m_new = jnp.maximum(m_old, jnp.max(top, axis=0, keepdims=True))
            alpha = jnp.exp2((m_old - m_new) * score_mul)
            total = l_s[h] * alpha
            added = None
            for b in range(blocks):
                s = sbuf[h % 2, b * kb:(b + 1) * kb].reshape(kb // 8, 8, pair)
                p = jnp.exp2((s - m_new[None]) * score_mul)
                total = total + jnp.sum(p, axis=0)
                v_t = jnp.concatenate([v_view[b * kb + i * hd:b * kb + (i + 1) * hd] for i in range(kb // hd)], axis=1)
                part = jnp.dot(v_t, p.reshape(kb, pair).astype(BF16), preferred_element_type=F32)
                added = part if added is None else added + part
            acc[h] = (acc[h].reshape(hd // 8, 8, pair) * alpha[None]).reshape(hd, pair) + added
            l_s[h] = total
            m_s[h] = m_new
            top = top_next

    def new_arrive(layer, u):
        src, direction = new_piece(u)
        new_copy(layer, src, u, direction).wait_recv()

        @pl.when((u < n_new - 3) | (u == n_new - 3))
        def _():
            new_copy(layer, src, u + 2, direction).start()

        @pl.when(src < z)
        def _():
            attend(nkv.at[layer, src, 0], nkv.at[layer, src, 1], False)

    def clear():
        def one_head(h, carry):
            m_s[h] = jnp.full(m_s.shape[1:], -jnp.inf, F32)
            l_s[h] = jnp.zeros(l_s.shape[1:], F32)
            acc[h] = jnp.zeros(acc.shape[1:], F32)
            return carry
        lax.fori_loop(0, heads_dev, one_head, 0)

    def rope(vals):
        rounded = vals.astype(BF16).astype(F32)
        return rounded * cos_ref[...] + pltpu.roll(rounded, hd // 2, 1) * sin_ref[...]

    def rotation():
        base = base_rot[z]
        cos_ref[...] = base[0:1] * local_rot[0] - base[1:2] * local_rot[1]
        sin_ref[...] = base[3:4] * local_rot[0] + base[2:3] * local_rot[1]

    def project(layer):
        proj = jnp.dot(xb[...], wqkv[...], preferred_element_type=F32)
        start = layer * (bias_ref.shape[0] // 2)
        for h in range(heads_dev):
            cols = slice(h * hd, (h + 1) * hd)
            qb[h] = rope(proj[:, cols] + bias_ref[pl.ds(start + c * heads_dev + h, 1)]).T.astype(BF16)
        k_rot = rope(proj[:, half:half + hd] + bias_ref[pl.ds(start + 2 * heads_dev + c, 1)]).astype(BF16)
        nkv[layer, z, 0] = k_rot
        knew[layer] = k_rot
        v_val = proj[:, half + hd:]
        vnew[layer] = v_val.astype(BF16)
        for i in range(pair // hd):
            nkv[layer, z, 1, i * hd:(i + 1) * hd] = v_val[i * hd:(i + 1) * hd].T.astype(BF16)

    def append_swap(layer, j):
        return pltpu.make_async_remote_copy((knew, vnew)[j].at[layer, other_rows], app_in.at[layer, j],
                                            d2d_s.at[8 + 2 * layer + j], d2d_r.at[8 + 2 * layer + j], device_id={"cp": partner})

    def send_new(layer):
        for direction in range(2):
            new_copy(layer, z, direction, direction).start()
        for j in range(2):
            append_swap(layer, j).start()

    def put_append(layer):
        return pltpu.make_async_copy(app_buf.at[layer], app_out.at[layer], loc.at[9 + layer])

    def append(layer):
        for j in range(2):
            append_swap(layer, j).wait_recv()
            mine = (knew, vnew)[j][layer, own_rows].astype(F32)
            theirs = app_in[layer, j].astype(F32)
            wide[pl.ds(0, tok, stride=2)] = jnp.where(c == 0, mine, theirs)
            wide[pl.ds(1, tok, stride=2)] = jnp.where(c == 0, theirs, mine)
            app_buf[layer, j] = wide[pl.ds(0, 2 * tok)].astype(BF16)
        put_append(layer).start()

    def finish_heads(layer):
        for h in range(heads_dev):
            total = jnp.sum(l_s[h], axis=0, keepdims=True)
            ob[layer, c, :, h * hd:(h + 1) * hd] = (acc[h] / total).T.astype(BF16)

    def attend_layer(layer):
        def step(s, carry):
            if layer == 0:
                @pl.when(s == n_steps - 2)
                def _():
                    send_own(1, 0)
                    send_own(1, 1)

                @pl.when(s >= 2)
                def _():
                    arrive(0, s - 2)
            else:
                @pl.when((s >= 2) & (s < 6))
                def _():
                    arrive(1, s + 2)

                @pl.when(s >= 10)
                def _():
                    arrive(1, s - 2)
            own = 1 - lax.div(s + n_steps - 2, n_steps)
            src, piece, _ = piece_of(lax.rem(s + n_steps - 2, n_steps))
            src = own * z + (1 - own) * src
            piece = own * lax.rem(c + s, 2) + (1 - own) * piece
            attend(kv.at[layer, src, piece, 0], kv.at[layer, src, piece, 1], False)

            @pl.when((s == 5) | (s == 9) | (s == 13) | (s == n_steps - 1))
            def _():
                last = lax.div(s, n_steps - 1)
                lo = lax.div(s - 5, 2) + last

                def new_step(u, carry):
                    new_arrive(layer, u)
                    return carry
                lax.fori_loop(lo, lo + 2 - last, new_step, 0)
            return carry

        lax.fori_loop(0, n_steps, step, 0)

    def span(body, lo, hi):
        def step(i, carry):
            body(i)
            return carry
        lax.fori_loop(lo, hi, step, 0)

    for j in range(2):
        load_cache(0, j).wait()
    split_cache(0)
    swap_cache(0).start()
    send_own(0, 0)
    for j in range(2):
        load_cache(1, j).start()
    rotation()
    swap_cache(0).wait_recv()
    send_own(0, 1)
    load_x.wait()
    swap_x.wait_recv()
    for cpy in load_wqkv(0):
        cpy.wait()
    project(0)
    send_new(0)
    load_wo(0).start()
    for cpy in load_wqkv(1):
        cpy.start()
    for slot in range(W_SLOTS):
        for cpy in load_ff(slot, slot):
            cpy.start()
    clear()
    attend(nkv.at[0, z, 0], nkv.at[0, z, 1], True)
    for j in range(2):
        load_cache(1, j).wait()
    split_cache(1)
    swap_cache(1).start()
    append(0)
    swap_cache(1).wait_recv()
    attend_layer(0)
    finish_heads(0)

    swap_o = pltpu.make_async_remote_copy(ob.at[0, c], ob.at[0, c], d2d_s.at[5], d2d_r.at[5], device_id={"cp": partner})
    swap_o.start()
    load_wo(0).wait()
    swap_o.wait_recv()
    y_one = (jnp.dot(ob[0, 0], wob[:half], preferred_element_type=F32)
             + jnp.dot(ob[0, 1], wob[half:], preferred_element_type=F32)).astype(BF16)
    h_val = (xb[...].astype(F32) + y_one.astype(F32)).astype(BF16)
    hb[...] = h_val
    xb[...] = rms_norm(h_val.astype(F32))
    load_wo(1).start()
    gacc[...] = jnp.zeros(gacc.shape, F32)

    def ff_step(i, carry):
        slot = lax.rem(i, W_SLOTS)
        for cpy in load_ff(i, slot):
            cpy.wait()
        both = jnp.dot(xb[...], w13[slot], preferred_element_type=F32).astype(BF16).astype(F32)
        gate = both[:, :FF_TILE]
        mixed = (gate * jax.nn.sigmoid(gate) * both[:, FF_TILE:]).astype(BF16)
        gacc[...] += jnp.dot(mixed, w2b[slot], preferred_element_type=F32)

        @pl.when(i + W_SLOTS < tiles)
        def _():
            for cpy in load_ff(i + W_SLOTS, slot):
                cpy.start()

        @pl.when(i == tiles // 2)
        def _():
            arrive(1, 0)
            arrive(1, 1)
        return carry

    lax.fori_loop(0, tiles, ff_step, 0)
    swap_g = pltpu.make_async_remote_copy(gacc, grecv, d2d_s.at[7], d2d_r.at[7], device_id={"cp": partner})
    swap_g.start()
    swap_g.wait_recv()
    g_val = (hb[...].astype(F32) + (gacc[...] + grecv[...])).astype(BF16)
    hb[...] = g_val
    put_g = pltpu.make_async_copy(hb.at[own_rows], g_out, loc.at[11])
    put_g.start()
    xb[...] = rms_norm(g_val.astype(F32))
    for cpy in load_wqkv(1):
        cpy.wait()
    project(1)
    span(lambda t: arrive(1, t), 2, 4)
    send_new(1)

    clear()
    attend(nkv.at[1, z, 0], nkv.at[1, z, 1], True)
    append(1)
    attend_layer(1)
    finish_heads(1)
    swap_y = pltpu.make_async_remote_copy(ob.at[1, c, other_rows], ob.at[1, c, other_rows], d2d_s.at[6], d2d_r.at[6],
                                          device_id={"cp": partner})
    swap_y.start()
    load_wo(1).wait()
    swap_y.wait_recv()
    ybuf[...] = (jnp.dot(ob[1, 0, own_rows], wob[:half], preferred_element_type=F32)
                 + jnp.dot(ob[1, 1, own_rows], wob[half:], preferred_element_type=F32)).astype(BF16)
    put_y = pltpu.make_async_copy(ybuf, y_out, loc.at[12])
    put_y.start()

    for layer in range(2):
        put_append(layer).wait()
        swap_cache(layer).wait_send()
        for j in range(2):
            append_swap(layer, j).wait_send()
        span(lambda t: ring_copy(layer, 0, 0, t, 0).wait_send(), 0, n_arr)
        span(lambda u: new_copy(layer, 0, u, 0).wait_send(), 0, n_new)
    swap_x.wait_send()
    swap_o.wait_send()
    swap_g.wait_send()
    swap_y.wait_send()
    put_g.wait()
    put_y.wait()


def rotation_tables(n, tok, cache_dev, hd):
    half_dim = hd // 2
    inv_freq = np.tile(ROPE_THETA ** (-np.arange(half_dim) * (2.0 / hd)), 2)
    pair = 2 * tok
    offset = np.arange(pair)[:, None] * inv_freq[None, :]
    base = (n * cache_dev + np.arange(n // 2) * pair)[:, None] * inv_freq[None, :]
    sign = np.where(np.arange(hd) < half_dim, -1.0, 1.0)[None, :]
    local_rot = np.stack([np.cos(offset), np.sin(offset)])
    base_rot = np.stack([np.cos(base), np.sin(base), sign * np.cos(base), sign * np.sin(base)], axis=1)
    return jnp.asarray(local_rot, F32), jnp.asarray(base_rot, F32)


def copy_kernel(g_in, y_in, app_in, g_out, y_out, *rest):
    app_outs, (g_buf, y_buf, app_buf, sems) = rest[:4], rest[4:]
    ins = [pltpu.make_async_copy(src, buf, sems.at[0, i]) for i, (src, buf) in enumerate(((y_in, y_buf), (g_in, g_buf), (app_in, app_buf)))]
    outs = [[pltpu.make_async_copy(y_buf, y_out, sems.at[1, 0])], [pltpu.make_async_copy(g_buf, g_out, sems.at[1, 1])],
            [pltpu.make_async_copy(app_buf.at[i // 2, i % 2], app_outs[i], sems.at[1, 2 + i]) for i in range(4)]]
    for cpy in ins:
        cpy.start()
    for cpy, group in zip(ins, outs):
        cpy.wait()
        for out in group:
            out.start()
    for group in outs:
        for out in group:
            out.wait()


def hand_over(hidden, y_two, app):
    any_spec = pl.BlockSpec(memory_space=pl.ANY)
    row_shape = jax.ShapeDtypeStruct(hidden.shape, hidden.dtype)
    app_shape = jax.ShapeDtypeStruct(app.shape[2:], app.dtype)
    return pl.pallas_call(
        copy_kernel,
        out_shape=[row_shape, row_shape] + [app_shape] * 4,
        in_specs=[any_spec] * 3,
        out_specs=[any_spec] * 6,
        scratch_shapes=[pltpu.VMEM(hidden.shape, BF16), pltpu.VMEM(hidden.shape, BF16), pltpu.VMEM(app.shape, BF16),
                        pltpu.SemaphoreType.DMA((2, 6))],
        name="hand_over",
    )(hidden, y_two, app)


def fused_blocks(n, x_in, cache, weights, biases, tables):
    tok, d_model = x_in.shape
    cache_dev, kv_heads, hd = cache[0].shape
    w_q1, w_gate = weights[0], weights[4]
    heads_dev = w_q1.shape[1] // hd // kv_heads
    half = heads_dev * hd
    nz = n // 2
    far = nz // 2
    n_arr = 4 * (far - 1) + 2
    n_new = 2 * (far - 1) + 1
    pair = 2 * tok
    rows = [arr.reshape(cache_dev * kv_heads, hd) for arr in cache]
    any_spec = pl.BlockSpec(memory_space=pl.ANY)
    vmem_spec = pl.BlockSpec(memory_space=pltpu.VMEM)
    dma = pltpu.SemaphoreType.DMA
    ff_half = w_gate.shape[1] // 2
    flops = 2 * pair * (d_model * (half + 2 * hd) * 2 + 3 * d_model * ff_half + 2 * half * d_model * 2) + 8 * pair * half * n * cache_dev
    return pl.pallas_call(
        functools.partial(block_kernel, n),
        out_shape=(jax.ShapeDtypeStruct((tok, d_model), BF16), jax.ShapeDtypeStruct((tok, d_model), BF16),
                   jax.ShapeDtypeStruct((2, 2, kv_heads * tok, hd), BF16)),
        in_specs=[any_spec] * 16 + [vmem_spec] * 3,
        out_specs=(any_spec, any_spec, any_spec),
        scratch_shapes=[
            pltpu.VMEM((2, nz, 2, 2, cache_dev, hd), BF16),
            pltpu.VMEM((2, nz, 2, pair, hd), BF16),
            pltpu.VMEM((2, 2, 2 * cache_dev, hd), BF16),
            pltpu.VMEM((2, 2, cache_dev, hd), BF16),
            pltpu.VMEM((2 * hd, hd), F32),
            pltpu.VMEM((2, cache_dev, pair), F32),
            pltpu.VMEM((pair, hd), F32),
            pltpu.VMEM((pair, hd), F32),
            pltpu.VMEM((2, pair, hd), BF16),
            pltpu.VMEM((2, pair, hd), BF16),
            pltpu.VMEM((2, 2, tok, hd), BF16),
            pltpu.VMEM((2, 2, pair, hd), BF16),
            pltpu.VMEM((pair, d_model), BF16),
            pltpu.VMEM((pair, d_model), BF16),
            pltpu.VMEM((heads_dev, hd, pair), BF16),
            pltpu.VMEM((heads_dev, hd, pair), F32),
            pltpu.VMEM((heads_dev, 8, pair), F32),
            pltpu.VMEM((heads_dev, 8, pair), F32),
            pltpu.VMEM((2, 2, pair, half), BF16),
            pltpu.VMEM((pair, d_model), F32),
            pltpu.VMEM((pair, d_model), F32),
            pltpu.VMEM((tok, d_model), BF16),
            pltpu.VMEM((d_model, half + 2 * hd), BF16),
            pltpu.VMEM((2 * half, d_model), BF16),
            pltpu.VMEM((W_SLOTS, d_model, 2 * FF_TILE), BF16),
            pltpu.VMEM((W_SLOTS, FF_TILE, d_model), BF16),
            dma((2, n_arr)), dma((2, n_arr)), dma((2, n_new)), dma((2, n_new)),
            dma((12,)), dma((12,)), dma((13,)), dma((W_SLOTS, 3)),
        ],
        compiler_params=pltpu.CompilerParams(collective_id=0, has_side_effects=True, vmem_limit_bytes=67043328),
        cost_estimate=pl.CostEstimate(flops=flops, bytes_accessed=6 * d_model * ff_half, transcendentals=0),
        name="fused_blocks",
    )(x_in, *rows, *weights, biases, *tables)


def solution(mesh):
    axis_size = mesh.shape['cp']
    rows_spec = P(('dp', 'cp'), None)
    cache_spec = P(('dp', 'cp'), None, None)
    mat_spec = P(None, None)
    vec_spec = P(None)
    layer_specs = (cache_spec, cache_spec, mat_spec, vec_spec, mat_spec, vec_spec, mat_spec, mat_spec)
    in_specs = (rows_spec,) + layer_specs + (mat_spec, mat_spec, mat_spec) + layer_specs
    out_specs = (rows_spec, rows_spec, cache_spec, cache_spec, cache_spec, cache_spec)

    def forward(x_in, cache_k1, cache_v1, w_q1, b_q1, w_k1, b_k1, w_v1, w_o1, w_gate, w_up, w_down, cache_k2, cache_v2, w_q2, b_q2, w_k2, b_k2, w_v2, w_o2):
        tok = x_in.shape[0]
        cache_dev, kv_heads, hd = cache_k1.shape
        tables = rotation_tables(axis_size, tok, cache_dev, hd)
        parts = (b_q1, b_k1, b_q2, b_k2)
        width = sum(part.shape[0] for part in parts)
        biases, start = 0.0, 0
        for part in parts:
            biases = biases + jnp.pad(part.astype(F32), (start, width - start - part.shape[0]))
            start += part.shape[0]
        biases = lax.optimization_barrier(biases).reshape(-1, hd)
        weights = (w_q1, w_k1, w_v1, w_o1, w_gate, w_up, w_down, w_q2, w_k2, w_v2, w_o2)
        hidden, y_two, app = fused_blocks(axis_size, x_in, (cache_k1, cache_v1, cache_k2, cache_v2), weights, biases, tables)
        outs = hand_over(hidden, y_two, app)
        return (outs[0], outs[1], *(arr.reshape(tok, kv_heads, hd) for arr in outs[2:]))

    return jax.shard_map(forward, mesh=mesh, in_specs=in_specs, out_specs=out_specs, check_vma=False)
```

```python
import functools

import jax
import jax.numpy as jnp
import numpy as np
from jax import lax
from jax.experimental import pallas as pl
from jax.experimental.pallas import tpu as pltpu
from jax.sharding import PartitionSpec as P

ROPE_THETA = 500000.0
NORM_EPS = 1e-5
LOG2E = 1.4426950408889634
BF16 = jnp.bfloat16
F32 = jnp.float32
FF_TILE = 640
W_SLOTS = 3
CORES = 2


def parity(i):
    return lax.rem(i, CORES)


def halve(i):
    return lax.div(i, CORES)


def repeat(count, body):
    lax.fori_loop(0, count, body, 0)


def product(left, right):
    return jnp.dot(left, right, preferred_element_type=F32)


def rms_norm(wide):
    return (wide * lax.rsqrt(jnp.mean(wide * wide, axis=-1, keepdims=True) + NORM_EPS)).astype(BF16)


def block_kernel(n, x_ref, kc1, vc1, kc2, vc2, wq1, wk1, wv1, wo1, wg, wu, wd, wq2, wk2, wv2, wo2, bias_ref, local_rot, base_rot,
                 g_out, y_out, app_out,
                 kv1, kv2, nk1, nk2, part_ml, far_acc, far_ml, raw, snd, wide, sbuf, cos_ref, sin_ref, knew, vnew, app_in, app_buf,
                 xb, hb, qb, acc, m_s, l_s, ob, gacc, grecv, ybuf, wqkv, wob, w13, w2b,
                 pair_s, pair_r, ring_s, ring_r, new_s, new_r, d2d_s, d2d_r, loc, wsem):
    nz = n // CORES
    far = nz // CORES
    n_arr = 4 * (far - 1) + 2
    n_new = 2 * (far - 1) + 1
    cp = lax.axis_index("cp")
    c = parity(cp)
    z = halve(cp)
    partner = cp + 1 - 2 * c
    odd = parity(z)
    mate = z + 1 - 2 * odd
    near = lax.rem(z + nz - 1 + 2 * odd, nz)
    tok = x_ref.shape[0]
    heads_dev = qb.shape[1]
    hd = qb.shape[2]
    pair = CORES * tok
    cache_dev = kv1.shape[3]
    n_steps = n_arr + 2
    half = heads_dev * hd
    ff_half = wg.shape[1] // 2
    tiles = ff_half // FF_TILE
    cache = (kc1, vc1), (kc2, vc2)
    wqkv_src = (wq1, wk1, wv1), (wq2, wk2, wv2)
    wo_src = (wo1, wo2)
    score_mul = hd ** -0.5 * LOG2E

    def toward(direction):
        return {"cp": lax.rem(cp + n + 2 - 4 * direction, n)}

    def chip(index):
        return {"cp": 2 * index + c}

    def own_slot(layer):
        return kv1.at[0] if layer == 0 else kv2.at[z]

    def own_new(layer):
        return nk1.at[0] if layer == 0 else nk2.at[z]

    def load_cache(layer, j):
        return pltpu.make_async_copy(cache[layer][j], raw.at[layer, j], loc.at[1 + 2 * layer + j])

    def swap_cache(layer):
        return pltpu.make_async_remote_copy(snd.at[layer], own_slot(layer).at[c], d2d_s.at[1 + layer], d2d_r.at[1 + layer],
                                            device_id={"cp": partner})

    def split_cache(layer):
        for j in range(CORES):
            def one_block(b, carry):
                wide[...] = raw[layer, j, pl.ds(pl.multiple_of(b * 2 * hd, 2 * hd), 2 * hd)].astype(F32)
                first = wide[pl.ds(0, hd, stride=2)]
                second = wide[pl.ds(1, hd, stride=2)]
                mine = jnp.where(c == 0, first, second)
                theirs = jnp.where(c == 0, second, first)
                if j == 1:
                    mine, theirs = mine.T, theirs.T
                rows = pl.ds(pl.multiple_of(b * hd, hd), hd)
                own_slot(layer)[c, j, rows] = mine.astype(BF16)
                snd[layer, j, rows] = theirs.astype(BF16)
                return carry
            repeat(cache_dev // hd, one_block)

    own_rows = pl.ds(pl.multiple_of(c * tok, tok), tok)
    other_rows = pl.ds(pl.multiple_of((1 - c) * tok, tok), tok)
    load_x = pltpu.make_async_copy(x_ref, xb.at[own_rows], loc.at[0])
    swap_x = pltpu.make_async_remote_copy(x_ref, xb.at[own_rows], d2d_s.at[0], d2d_r.at[0], device_id={"cp": partner})

    def load_wqkv(layer):
        w_q, w_k, w_v = wqkv_src[layer]
        return (pltpu.make_async_copy(w_q.at[:, pl.ds(pl.multiple_of(c * half, hd), half)], wqkv.at[:, pl.ds(0, half)], loc.at[5]),
                pltpu.make_async_copy(w_k.at[:, pl.ds(pl.multiple_of(c * hd, hd), hd)], wqkv.at[:, pl.ds(half, hd)], loc.at[6]),
                pltpu.make_async_copy(w_v.at[:, pl.ds(pl.multiple_of(c * hd, hd), hd)], wqkv.at[:, pl.ds(half + hd, hd)], loc.at[7]))

    def load_wo(layer):
        return pltpu.make_async_copy(wo_src[layer], wob, loc.at[8])

    def load_ff(tile, slot):
        cols = pl.ds(pl.multiple_of(c * ff_half + tile * FF_TILE, 128), FF_TILE)
        return (pltpu.make_async_copy(wg.at[:, cols], w13.at[slot, :, pl.ds(0, FF_TILE)], wsem.at[slot, 0]),
                pltpu.make_async_copy(wu.at[:, cols], w13.at[slot, :, pl.ds(FF_TILE, FF_TILE)], wsem.at[slot, 1]),
                pltpu.make_async_copy(wd.at[cols], w2b.at[slot], wsem.at[slot, 2]))


    hops = (None, (0, near), (4, near), (5, near), (0, mate), (1, mate))

    def pair_copy(slot, order):
        src, target = hops[slot]
        piece = parity(c + order)
        return pltpu.make_async_remote_copy(kv1.at[src, piece], kv1.at[slot, piece], pair_s.at[slot, order],
                                            pair_r.at[slot, order], device_id=chip(target))

    def pair_new(slot):
        src, target = hops[slot]
        return pltpu.make_async_remote_copy(nk1.at[src], nk1.at[slot], pair_s.at[slot, 2], pair_r.at[slot, 2], device_id=chip(target))

    def relay(slot, order, onto):
        pair_copy(slot, order).wait_recv()
        pair_copy(onto, order).start()

    def relay_new(slot, onto):
        pair_new(slot).wait_recv()
        pair_new(onto).start()

    swap_q = pltpu.make_async_remote_copy(qb.at[0], qb.at[1], pair_s.at[0, 0], pair_r.at[0, 0], device_id=chip(mate))
    swap_acc = pltpu.make_async_remote_copy(acc.at[1], far_acc, pair_s.at[0, 1], pair_r.at[0, 1], device_id=chip(mate))
    swap_ml = pltpu.make_async_remote_copy(part_ml, far_ml, pair_s.at[0, 2], pair_r.at[0, 2], device_id=chip(mate))

    def piece_of(t):
        dist = lax.div(t, 4) + 1
        r = lax.rem(t, 4)
        direction = parity(t)
        order = halve(r) + parity(r) * lax.div(dist, far)
        src = lax.rem(z + nz + dist * (2 * direction - 1), nz)
        return src, parity(c + order), direction

    def ring_copy(src, piece, t, direction):
        return pltpu.make_async_remote_copy(kv2.at[src, piece], kv2.at[src, piece], ring_s.at[t], ring_r.at[t],
                                            device_id=toward(direction))

    def send_own(direction, order):
        ring_copy(z, parity(c + order), 2 * order + direction, direction).start()

    def arrive(t):
        src, piece, direction = piece_of(t)
        ring_copy(src, piece, t, direction).wait_recv()
        last = 4 * (far - 1)

        @pl.when((t < last - 4) | (t == last - 4) | (t == last - 1))
        def _():
            ring_copy(src, piece, t + 4 - 2 * lax.div(t, last - 1), direction).start()

    def new_piece(u):
        dist = halve(u) + 1
        direction = parity(u)
        return lax.rem(z + dist * (2 * direction - 1) + nz, nz), direction

    def new_copy(src, u, direction):
        return pltpu.make_async_remote_copy(nk2.at[src], nk2.at[src], new_s.at[u], new_r.at[u], device_id=toward(direction))

    def attend(group, keys_values, causal=False):
        k_view, v_view = keys_values.at[0], keys_values.at[1]
        keys = k_view.shape[0]
        kb = min(256, keys)
        blocks = keys // kb

        def scores(h):
            top = None
            for b in range(blocks):
                s = product(k_view[b * kb:(b + 1) * kb], qb[group, h])
                if causal:
                    key = lax.broadcasted_iota(jnp.int32, s.shape, 0) + b * kb
                    query = lax.broadcasted_iota(jnp.int32, s.shape, 1)
                    s = jnp.where(key <= query, s, -jnp.inf)
                sbuf[h % 2, b * kb:(b + 1) * kb] = s
                part = jnp.max(s.reshape(kb // 8, 8, pair), axis=0)
                top = part if top is None else jnp.maximum(top, part)
            return top

        top = scores(0)
        for h in range(heads_dev):
            top_next = scores(h + 1) if h + 1 < heads_dev else None
            m_old = m_s[group, h]
            m_new = jnp.maximum(m_old, jnp.max(top, axis=0, keepdims=True))
            alpha = jnp.exp2((m_old - m_new) * score_mul)
            total = l_s[group, h] * alpha
            added = None
            for b in range(blocks):
                s = sbuf[h % 2, b * kb:(b + 1) * kb].reshape(kb // 8, 8, pair)
                p = jnp.exp2((s - m_new[None]) * score_mul)
                total = total + jnp.sum(p, axis=0)
                v_t = jnp.concatenate([v_view[b * kb + i * hd:b * kb + (i + 1) * hd] for i in range(kb // hd)], axis=1)
                part = product(v_t, p.reshape(kb, pair).astype(BF16))
                added = part if added is None else added + part
            acc[group, h] = (acc[group, h].reshape(hd // 8, 8, pair) * alpha[None]).reshape(hd, pair) + added
            l_s[group, h] = total
            m_s[group, h] = m_new
            top = top_next

    def new_arrive(u):
        src, direction = new_piece(u)
        new_copy(src, u, direction).wait_recv()

        @pl.when((u < n_new - 3) | (u == n_new - 3))
        def _():
            new_copy(src, u + 2, direction).start()

        @pl.when(src < z)
        def _():
            attend(0, nk2.at[src])

    def clear(groups):
        def one(i, carry):
            group, h = lax.div(i, heads_dev), lax.rem(i, heads_dev)
            m_s[group, h] = jnp.full(m_s.shape[2:], -jnp.inf, F32)
            l_s[group, h] = jnp.zeros(l_s.shape[2:], F32)
            acc[group, h] = jnp.zeros(acc.shape[2:], F32)
            return carry
        repeat(groups * heads_dev, one)

    def rope(vals):
        rounded = vals.astype(BF16).astype(F32)
        return rounded * cos_ref[...] + pltpu.roll(rounded, hd // 2, 1) * sin_ref[...]

    def rotation():
        base = base_rot[z]
        cos_ref[...] = base[0:1] * local_rot[0] - base[1:2] * local_rot[1]
        sin_ref[...] = base[3:4] * local_rot[0] + base[2:3] * local_rot[1]

    def project(layer):
        proj = product(xb[...], wqkv[...])
        start = layer * (bias_ref.shape[0] // 2)
        for h in range(heads_dev):
            cols = slice(h * hd, (h + 1) * hd)
            qb[0, h] = rope(proj[:, cols] + bias_ref[pl.ds(start + c * heads_dev + h, 1)]).T.astype(BF16)
        k_rot = rope(proj[:, half:half + hd] + bias_ref[pl.ds(start + 2 * heads_dev + c, 1)]).astype(BF16)
        own_new(layer)[0] = k_rot
        knew[layer] = k_rot
        v_val = proj[:, half + hd:]
        vnew[layer] = v_val.astype(BF16)
        for i in range(pair // hd):
            own_new(layer)[1, i * hd:(i + 1) * hd] = v_val[i * hd:(i + 1) * hd].T.astype(BF16)

    def append_swap(layer, j):
        return pltpu.make_async_remote_copy((knew, vnew)[j].at[layer, other_rows], app_in.at[layer, j],
                                            d2d_s.at[8 + 2 * layer + j], d2d_r.at[8 + 2 * layer + j], device_id={"cp": partner})

    def send_append(layer):
        for j in range(CORES):
            append_swap(layer, j).start()

    def put_append(layer):
        return pltpu.make_async_copy(app_buf.at[layer], app_out.at[layer], loc.at[9 + layer])

    def append(layer):
        for j in range(CORES):
            append_swap(layer, j).wait_recv()
            mine = (knew, vnew)[j][layer, own_rows].astype(F32)
            theirs = app_in[layer, j].astype(F32)
            wide[pl.ds(0, tok, stride=2)] = jnp.where(c == 0, mine, theirs)
            wide[pl.ds(1, tok, stride=2)] = jnp.where(c == 0, theirs, mine)
            app_buf[layer, j] = wide[pl.ds(0, 2 * tok)].astype(BF16)
        put_append(layer).start()

    def finish_heads(layer):
        for h in range(heads_dev):
            total = jnp.sum(l_s[0, h], axis=0, keepdims=True)
            summed = acc[0, h]
            if layer == 0:
                m_own, m_far = m_s[0, h, 0:1], far_ml[h:h + 1]
                m_all = jnp.maximum(m_own, m_far)
                w_own, w_far = jnp.exp2((m_own - m_all) * score_mul), jnp.exp2((m_far - m_all) * score_mul)
                total = total * w_own + far_ml[8 + h:9 + h] * w_far
                summed = summed * w_own + far_acc[h] * w_far
            ob[layer, c, :, h * hd:(h + 1) * hd] = (summed / total).T.astype(BF16)

    def hand_back():
        for h in range(heads_dev):
            part_ml[h:h + 1] = m_s[1, h, 0:1]
            part_ml[8 + h:9 + h] = jnp.sum(l_s[1, h], axis=0, keepdims=True)
        swap_acc.start()
        swap_ml.start()

    def attend_first():
        def step(k, carry):
            @pl.when(k == 2)
            def _():
                relay(1, 0, 5)
                relay(4, 0, 2)
                relay_new(1, 5)
                relay_new(4, 2)

            @pl.when(k == 3)
            def _():
                swap_q.wait_recv()

            @pl.when(k == 6)
            def _():
                relay(1, 1, 5)

            @pl.when(k == 8)
            def _():
                relay(4, 1, 2)
                pair_copy(2, 0).wait_recv()

            @pl.when(k == 10)
            def _():
                relay(5, 0, 3)
                pair_copy(2, 1).wait_recv()
                pair_new(2).wait_recv()
                relay_new(5, 3)

            @pl.when(k == 12)
            def _():
                relay(5, 1, 3)
                for direction in (odd, 1 - odd):
                    for order in range(CORES):
                        send_own(direction, order)

            @pl.when(k == 14)
            def _():
                pair_new(3).wait_recv()

            @pl.when((k == 12) | (k == 14))
            def _():
                turn = halve(k - 12)

                def new_step(i, carry):
                    slot, group = halve(i), parity(i)
                    src = lax.rem(z + nz + slot * (2 * odd - 1), nz)

                    @pl.when(src < (1 - group) * z + group * mate)
                    def _():
                        attend(group, nk1.at[slot])
                    return carry
                lax.fori_loop(6 * turn, 6 + 2 * turn, new_step, 0)

            @pl.when(k == 12)
            def _():
                pair_copy(3, 0).wait_recv()

            @pl.when(k == 14)
            def _():
                pair_copy(3, 1).wait_recv()

            @pl.when(k == 15)
            def _():
                hand_back()

            early = 1 - lax.div(k + 10, 16)
            i, end = lax.rem(k, 3), lax.div(k, 12)
            slot = early * halve(i) + (1 - early) * lax.div(k, 4)
            order = early * parity(i) + (1 - early) * lax.rem(halve(k), 2)
            group = early * lax.div(k, 3) + (1 - early) * (parity(k) * (1 - 2 * end) + end)
            piece = parity(c + order)
            attend(group, kv1.at[slot, piece])
            return carry

        repeat(16, step)

    def attend_second():
        def step(s, carry):
            @pl.when((s == 2) | (s == 3))
            def _():
                arrive(s + 4)

            @pl.when((s == 8) | (s == 9))
            def _():
                arrive(s)

            @pl.when(s >= 12)
            def _():
                arrive(s - 2)
            own = 1 - lax.div(s + n_steps - 2, n_steps)
            src, piece, _ = piece_of(lax.rem(s + n_steps - 2, n_steps))
            src = own * z + (1 - own) * src
            piece = own * parity(c + s) + (1 - own) * piece
            attend(0, kv2.at[src, piece])

            @pl.when((s == 5) | (s == 11) | (s == 13) | (s == n_steps - 1))
            def _():
                last = lax.div(s, n_steps - 1)
                lo = (s - 9) * lax.div(s, 11)

                def new_step(u, carry):
                    new_arrive(u)
                    return carry
                lax.fori_loop(lo, lo + 2 - last, new_step, 0)
            return carry

        repeat(n_steps, step)

    def span(body, lo, hi):
        def step(i, carry):
            body(i)
            return carry
        lax.fori_loop(lo, hi, step, 0)

    for j in range(CORES):
        load_cache(0, j).start()
    load_x.start()
    for cpy in load_wqkv(0):
        cpy.start()
    barrier = pltpu.get_barrier_semaphore()
    for other in (partner, 2 * mate + c, 2 * near + c):
        pl.semaphore_signal(barrier, inc=1, device_id={"cp": other})
    for j in range(CORES):
        load_cache(0, j).wait()
    split_cache(0)
    pl.semaphore_wait(barrier, 3)
    for slot in (1, 4):
        pair_copy(slot, 0).start()
    swap_cache(0).start()
    swap_x.start()
    for j in range(CORES):
        load_cache(1, j).start()
    rotation()
    load_x.wait()
    swap_x.wait_recv()
    for cpy in load_wqkv(0):
        cpy.wait()
    project(0)
    for slot in (1, 4):
        pair_new(slot).start()
    swap_q.start()
    swap_cache(0).wait_recv()
    for slot in (1, 4):
        pair_copy(slot, 1).start()
    send_append(0)
    load_wo(0).start()
    for cpy in load_wqkv(1):
        cpy.start()
    for slot in range(W_SLOTS):
        for cpy in load_ff(slot, slot):
            cpy.start()
    clear(2)
    attend(0, nk1.at[0], causal=True)
    for j in range(CORES):
        load_cache(1, j).wait()
    split_cache(1)
    swap_cache(1).start()
    append(0)
    swap_cache(1).wait_recv()
    attend_first()
    span(arrive, 0, 2)
    swap_acc.wait_recv()
    swap_ml.wait_recv()
    finish_heads(0)

    swap_o = pltpu.make_async_remote_copy(ob.at[0, c], ob.at[0, c], d2d_s.at[5], d2d_r.at[5], device_id={"cp": partner})
    swap_o.start()
    load_wo(0).wait()
    swap_o.wait_recv()
    y_one = (product(ob[0, 0], wob[:half])
             + product(ob[0, 1], wob[half:])).astype(BF16)
    h_val = (xb[...].astype(F32) + y_one.astype(F32)).astype(BF16)
    hb[...] = h_val
    xb[...] = rms_norm(h_val.astype(F32))
    load_wo(1).start()
    gacc[...] = jnp.zeros(gacc.shape, F32)

    def ff_step(i, carry):
        slot = lax.rem(i, W_SLOTS)
        for cpy in load_ff(i, slot):
            cpy.wait()
        both = product(xb[...], w13[slot]).astype(BF16).astype(F32)
        gate = both[:, :FF_TILE]
        mixed = (gate * jax.nn.sigmoid(gate) * both[:, FF_TILE:]).astype(BF16)
        gacc[...] += product(mixed, w2b[slot])

        @pl.when(i == tiles - 3)
        def _():
            span(arrive, 2, 4)

        @pl.when(i + W_SLOTS < tiles)
        def _():
            for cpy in load_ff(i + W_SLOTS, slot):
                cpy.start()
        return carry

    repeat(tiles, ff_step)
    swap_g = pltpu.make_async_remote_copy(gacc, grecv, d2d_s.at[7], d2d_r.at[7], device_id={"cp": partner})
    swap_g.start()
    span(arrive, 4, 6)
    swap_g.wait_recv()
    g_val = (hb[...].astype(F32) + (gacc[...] + grecv[...])).astype(BF16)
    hb[...] = g_val
    put_g = pltpu.make_async_copy(hb.at[own_rows], g_out, loc.at[11])
    put_g.start()
    xb[...] = rms_norm(g_val.astype(F32))
    for cpy in load_wqkv(1):
        cpy.wait()
    swap_q.wait_send()
    project(1)
    for direction in range(CORES):
        new_copy(z, direction, direction).start()
    send_append(1)

    clear(1)
    attend(0, nk2.at[z], causal=True)
    append(1)
    attend_second()
    finish_heads(1)
    swap_y = pltpu.make_async_remote_copy(ob.at[1, c, other_rows], ob.at[1, c, other_rows], d2d_s.at[6], d2d_r.at[6],
                                          device_id={"cp": partner})
    swap_y.start()
    load_wo(1).wait()
    swap_y.wait_recv()
    ybuf[...] = (product(ob[1, 0, own_rows], wob[:half])
                 + product(ob[1, 1, own_rows], wob[half:])).astype(BF16)
    put_y = pltpu.make_async_copy(ybuf, y_out, loc.at[12])
    put_y.start()

    for layer in range(CORES):
        put_append(layer).wait()
        swap_cache(layer).wait_send()
        for j in range(CORES):
            append_swap(layer, j).wait_send()
    span(lambda t: ring_copy(0, 0, t, 0).wait_send(), 0, n_arr)
    span(lambda u: new_copy(0, u, 0).wait_send(), 0, n_new)
    for slot in range(1, 6):
        for order in range(CORES):
            pair_copy(slot, order).wait_send()
        pair_new(slot).wait_send()
    swap_acc.wait_send()
    swap_ml.wait_send()
    swap_x.wait_send()
    swap_o.wait_send()
    swap_g.wait_send()
    swap_y.wait_send()
    put_g.wait()
    put_y.wait()


def rotation_tables(n, tok, cache_dev, hd):
    half_dim = hd // 2
    inv_freq = np.tile(ROPE_THETA ** (-np.arange(half_dim) * (2.0 / hd)), 2)
    pair = CORES * tok
    offset = np.arange(pair)[:, None] * inv_freq[None, :]
    base = (n * cache_dev + np.arange(n // 2) * pair)[:, None] * inv_freq[None, :]
    sign = np.where(np.arange(hd) < half_dim, -1.0, 1.0)[None, :]
    local_rot = np.stack([np.cos(offset), np.sin(offset)])
    base_rot = np.stack([np.cos(base), np.sin(base), sign * np.cos(base), sign * np.sin(base)], axis=1)
    return jnp.asarray(local_rot, F32), jnp.asarray(base_rot, F32)


def copy_kernel(g_in, y_in, app_in, g_out, y_out, *rest):
    app_outs, (g_buf, y_buf, app_buf, sems) = rest[:4], rest[4:]
    ins = [pltpu.make_async_copy(src, buf, sems.at[0, i]) for i, (src, buf) in enumerate(((y_in, y_buf), (g_in, g_buf), (app_in, app_buf)))]
    outs = [[pltpu.make_async_copy(y_buf, y_out, sems.at[1, 0])], [pltpu.make_async_copy(g_buf, g_out, sems.at[1, 1])],
            [pltpu.make_async_copy(app_buf.at[i // 2, i % 2], app_outs[i], sems.at[1, 2 + i]) for i in range(4)]]
    for cpy in ins:
        cpy.start()
    for cpy, group in zip(ins, outs):
        cpy.wait()
        for out in group:
            out.start()
    for group in outs:
        for out in group:
            out.wait()


def hand_over(hidden, y_two, app):
    any_spec = pl.BlockSpec(memory_space=pl.ANY)
    row_shape = jax.ShapeDtypeStruct(hidden.shape, hidden.dtype)
    app_shape = jax.ShapeDtypeStruct(app.shape[2:], app.dtype)
    return pl.pallas_call(
        copy_kernel,
        out_shape=[row_shape, row_shape] + [app_shape] * 4,
        in_specs=[any_spec] * 3,
        out_specs=[any_spec] * 6,
        scratch_shapes=[pltpu.VMEM(hidden.shape, BF16), pltpu.VMEM(hidden.shape, BF16), pltpu.VMEM(app.shape, BF16),
                        pltpu.SemaphoreType.DMA((2, 6))],
        name="hand_over",
    )(hidden, y_two, app)


def fused_blocks(n, x_in, cache, weights, biases, tables):
    tok, d_model = x_in.shape
    cache_dev, kv_heads, hd = cache[0].shape
    w_q1, w_gate = weights[0], weights[4]
    heads_dev = w_q1.shape[1] // hd // kv_heads
    half = heads_dev * hd
    nz = n // CORES
    far = nz // CORES
    n_arr = 4 * (far - 1) + 2
    n_new = 2 * (far - 1) + 1
    pair = CORES * tok
    rows = [arr.reshape(cache_dev * kv_heads, hd) for arr in cache]
    any_spec = pl.BlockSpec(memory_space=pl.ANY)
    vmem_spec = pl.BlockSpec(memory_space=pltpu.VMEM)
    dma = pltpu.SemaphoreType.DMA
    ff_half = w_gate.shape[1] // 2
    flops = 2 * pair * (d_model * (half + 2 * hd) * 2 + 3 * d_model * ff_half + 2 * half * d_model * 2) + 8 * pair * half * n * cache_dev
    return pl.pallas_call(
        functools.partial(block_kernel, n),
        out_shape=(jax.ShapeDtypeStruct((tok, d_model), BF16), jax.ShapeDtypeStruct((tok, d_model), BF16),
                   jax.ShapeDtypeStruct((2, 2, kv_heads * tok, hd), BF16)),
        in_specs=[any_spec] * 16 + [vmem_spec] * 3,
        out_specs=(any_spec, any_spec, any_spec),
        scratch_shapes=[
            pltpu.VMEM((6, 2, 2, cache_dev, hd), BF16),
            pltpu.VMEM((nz, 2, 2, cache_dev, hd), BF16),
            pltpu.VMEM((6, 2, pair, hd), BF16),
            pltpu.VMEM((nz, 2, pair, hd), BF16),
            pltpu.VMEM((16, pair), F32),
            pltpu.VMEM((heads_dev, hd, pair), F32),
            pltpu.VMEM((16, pair), F32),
            pltpu.VMEM((CORES, CORES, 2 * cache_dev, hd), BF16),
            pltpu.VMEM((CORES, CORES, cache_dev, hd), BF16),
            pltpu.VMEM((2 * hd, hd), F32),
            pltpu.VMEM((CORES, cache_dev, pair), F32),
            pltpu.VMEM((pair, hd), F32),
            pltpu.VMEM((pair, hd), F32),
            pltpu.VMEM((CORES, pair, hd), BF16),
            pltpu.VMEM((CORES, pair, hd), BF16),
            pltpu.VMEM((CORES, CORES, tok, hd), BF16),
            pltpu.VMEM((CORES, CORES, pair, hd), BF16),
            pltpu.VMEM((pair, d_model), BF16),
            pltpu.VMEM((pair, d_model), BF16),
            pltpu.VMEM((CORES, heads_dev, hd, pair), BF16),
            pltpu.VMEM((CORES, heads_dev, hd, pair), F32),
            pltpu.VMEM((CORES, heads_dev, 8, pair), F32),
            pltpu.VMEM((CORES, heads_dev, 8, pair), F32),
            pltpu.VMEM((CORES, CORES, pair, half), BF16),
            pltpu.VMEM((pair, d_model), F32),
            pltpu.VMEM((pair, d_model), F32),
            pltpu.VMEM((tok, d_model), BF16),
            pltpu.VMEM((d_model, half + 2 * hd), BF16),
            pltpu.VMEM((2 * half, d_model), BF16),
            pltpu.VMEM((W_SLOTS, d_model, 2 * FF_TILE), BF16),
            pltpu.VMEM((W_SLOTS, FF_TILE, d_model), BF16),
            dma((6, 3)), dma((6, 3)), dma((n_arr,)), dma((n_arr,)), dma((n_new,)), dma((n_new,)),
            dma((12,)), dma((12,)), dma((13,)), dma((W_SLOTS, 3)),
        ],
        compiler_params=pltpu.CompilerParams(collective_id=0, has_side_effects=True, vmem_limit_bytes=67043328),
        cost_estimate=pl.CostEstimate(flops=flops, bytes_accessed=6 * d_model * ff_half, transcendentals=0),
        name="fused_blocks",
    )(x_in, *rows, *weights, biases, *tables)


def solution(mesh):
    axis_size = mesh.shape['cp']
    rows_spec = P(('dp', 'cp'), None)
    cache_spec = P(('dp', 'cp'), None, None)
    mat_spec = P(None, None)
    vec_spec = P(None)
    layer_specs = (cache_spec, cache_spec, mat_spec, vec_spec, mat_spec, vec_spec, mat_spec, mat_spec)
    in_specs = (rows_spec,) + layer_specs + (mat_spec, mat_spec, mat_spec) + layer_specs
    out_specs = (rows_spec, rows_spec, cache_spec, cache_spec, cache_spec, cache_spec)

    def forward(x_in, cache_k1, cache_v1, w_q1, b_q1, w_k1, b_k1, w_v1, w_o1, w_gate, w_up, w_down, cache_k2, cache_v2, w_q2, b_q2, w_k2, b_k2, w_v2, w_o2):
        tok = x_in.shape[0]
        cache_dev, kv_heads, hd = cache_k1.shape
        tables = rotation_tables(axis_size, tok, cache_dev, hd)
        parts = (b_q1, b_k1, b_q2, b_k2)
        width = sum(part.shape[0] for part in parts)
        biases, start = 0.0, 0
        for part in parts:
            biases = biases + jnp.pad(part.astype(F32), (start, width - start - part.shape[0]))
            start += part.shape[0]
        biases = lax.optimization_barrier(biases).reshape(-1, hd)
        weights = (w_q1, w_k1, w_v1, w_o1, w_gate, w_up, w_down, w_q2, w_k2, w_v2, w_o2)
        hidden, y_two, app = fused_blocks(axis_size, x_in, (cache_k1, cache_v1, cache_k2, cache_v2), weights, biases, tables)
        outs = hand_over(hidden, y_two, app)
        return (outs[0], outs[1], *(arr.reshape(tok, kv_heads, hd) for arr in outs[2:]))

    return jax.shard_map(forward, mesh=mesh, in_specs=in_specs, out_specs=out_specs, check_vma=False)
```

```python
import functools

import jax
import jax.numpy as jnp
import numpy as np
from jax import lax
from jax.experimental import pallas as pl
from jax.experimental.pallas import tpu as pltpu
from jax.sharding import PartitionSpec as P

ROPE_THETA = 500000.0
NORM_EPS = 1e-5
LOG2E = 1.4426950408889634
BF16 = jnp.bfloat16
F32 = jnp.float32
FF_TILE = 640
W_SLOTS = 3
CORES = 2


def parity(i):
    return lax.rem(i, CORES)


def halve(i):
    return lax.div(i, CORES)


def repeat(count, body):
    lax.fori_loop(0, count, body, 0)


def product(left, right):
    return jnp.dot(left, right, preferred_element_type=F32)


def rms_norm(wide):
    return (wide * lax.rsqrt(jnp.mean(wide * wide, axis=-1, keepdims=True) + NORM_EPS)).astype(BF16)


def block_kernel(n, x_ref, kc1, vc1, kc2, vc2, wq1, wk1, wv1, wo1, wg, wu, wd, wq2, wk2, wv2, wo2, bq1, bk1, bq2, bk2, local_rot, base_rot,
                 g_out, y_out, app_out,
                 kv1, kv2, nk1, nk2, part_ml, far_acc, far_ml, raw, snd, wide, sbuf, cos_ref, sin_ref, knew, vnew, app_in, app_buf,
                 xb, hb, qb, acc, m_s, l_s, ob, gacc, grecv, ybuf, wqkv, wob, w13, w2b,
                 pair_s, pair_r, ring_s, ring_r, new_s, new_r, d2d_s, d2d_r, loc, wsem):
    nz = n // CORES
    far = nz // CORES
    n_arr = 4 * (far - 1) + 2
    n_new = 2 * (far - 1) + 1
    cp = lax.axis_index("cp")
    c = parity(cp)
    z = halve(cp)
    partner = cp + 1 - 2 * c
    odd = parity(z)
    mate = z + 1 - 2 * odd
    near = lax.rem(z + nz - 1 + 2 * odd, nz)
    tok = x_ref.shape[0]
    heads_dev = qb.shape[1]
    hd = qb.shape[2]
    pair = CORES * tok
    cache_dev = kv1.shape[3]
    n_steps = n_arr + 2
    half = heads_dev * hd
    ff_half = wg.shape[1] // 2
    tiles = ff_half // FF_TILE
    cache = (kc1, vc1), (kc2, vc2)
    wqkv_src = (wq1, wk1, wv1), (wq2, wk2, wv2)
    wo_src = (wo1, wo2)
    score_mul = hd ** -0.5 * LOG2E

    def toward(direction):
        return {"cp": lax.rem(cp + n + 2 - 4 * direction, n)}

    def chip(index):
        return {"cp": 2 * index + c}

    def own_slot(layer):
        return kv1.at[0] if layer == 0 else kv2.at[z]

    def own_new(layer):
        return nk1.at[0] if layer == 0 else nk2.at[z]

    def load_cache(layer, j):
        return pltpu.make_async_copy(cache[layer][j], raw.at[layer, j], loc.at[1 + 2 * layer + j])

    def swap_cache(layer):
        return pltpu.make_async_remote_copy(snd.at[layer], own_slot(layer).at[c], d2d_s.at[1 + layer], d2d_r.at[1 + layer],
                                            device_id={"cp": partner})

    def split_cache(layer):
        for j in range(CORES):
            def one_block(b, carry):
                wide[...] = raw[layer, j, pl.ds(pl.multiple_of(b * 2 * hd, 2 * hd), 2 * hd)].astype(F32)
                first = wide[pl.ds(0, hd, stride=2)]
                second = wide[pl.ds(1, hd, stride=2)]
                mine = jnp.where(c == 0, first, second)
                theirs = jnp.where(c == 0, second, first)
                if j == 1:
                    mine, theirs = mine.T, theirs.T
                rows = pl.ds(pl.multiple_of(b * hd, hd), hd)
                own_slot(layer)[c, j, rows] = mine.astype(BF16)
                snd[layer, j, rows] = theirs.astype(BF16)
                return carry
            repeat(cache_dev // hd, one_block)

    own_rows = pl.ds(pl.multiple_of(c * tok, tok), tok)
    other_rows = pl.ds(pl.multiple_of((1 - c) * tok, tok), tok)
    load_x = pltpu.make_async_copy(x_ref, xb.at[own_rows], loc.at[0])
    swap_x = pltpu.make_async_remote_copy(x_ref, xb.at[own_rows], d2d_s.at[0], d2d_r.at[0], device_id={"cp": partner})

    def load_wqkv(layer):
        w_q, w_k, w_v = wqkv_src[layer]
        return (pltpu.make_async_copy(w_q.at[:, pl.ds(pl.multiple_of(c * half, hd), half)], wqkv.at[:, pl.ds(0, half)], loc.at[5]),
                pltpu.make_async_copy(w_k.at[:, pl.ds(pl.multiple_of(c * hd, hd), hd)], wqkv.at[:, pl.ds(half, hd)], loc.at[6]),
                pltpu.make_async_copy(w_v.at[:, pl.ds(pl.multiple_of(c * hd, hd), hd)], wqkv.at[:, pl.ds(half + hd, hd)], loc.at[7]))

    def load_wo(layer):
        return pltpu.make_async_copy(wo_src[layer], wob, loc.at[8])

    def load_ff(tile, slot):
        cols = pl.ds(pl.multiple_of(c * ff_half + tile * FF_TILE, 128), FF_TILE)
        return (pltpu.make_async_copy(wg.at[:, cols], w13.at[slot, :, pl.ds(0, FF_TILE)], wsem.at[slot, 0]),
                pltpu.make_async_copy(wu.at[:, cols], w13.at[slot, :, pl.ds(FF_TILE, FF_TILE)], wsem.at[slot, 1]),
                pltpu.make_async_copy(wd.at[cols], w2b.at[slot], wsem.at[slot, 2]))


    hops = (None, (0, near), (4, near), (5, near), (0, mate), (1, mate))

    def pair_copy(slot, order):
        src, target = hops[slot]
        piece = parity(c + order)
        return pltpu.make_async_remote_copy(kv1.at[src, piece], kv1.at[slot, piece], pair_s.at[slot, order],
                                            pair_r.at[slot, order], device_id=chip(target))

    def pair_new(slot):
        src, target = hops[slot]
        return pltpu.make_async_remote_copy(nk1.at[src], nk1.at[slot], pair_s.at[slot, 2], pair_r.at[slot, 2], device_id=chip(target))

    def relay(slot, order, onto):
        pair_copy(slot, order).wait_recv()
        pair_copy(onto, order).start()

    def relay_new(slot, onto):
        pair_new(slot).wait_recv()
        pair_new(onto).start()

    swap_q = pltpu.make_async_remote_copy(qb.at[0], qb.at[1], pair_s.at[0, 0], pair_r.at[0, 0], device_id=chip(mate))
    swap_acc = pltpu.make_async_remote_copy(acc.at[1], far_acc, pair_s.at[0, 1], pair_r.at[0, 1], device_id=chip(mate))
    swap_ml = pltpu.make_async_remote_copy(part_ml, far_ml, pair_s.at[0, 2], pair_r.at[0, 2], device_id=chip(mate))

    def piece_of(t):
        dist = lax.div(t, 4) + 1
        r = lax.rem(t, 4)
        direction = parity(t)
        order = halve(r) + parity(r) * lax.div(dist, far)
        src = lax.rem(z + nz + dist * (2 * direction - 1), nz)
        return src, parity(c + order), direction

    def ring_copy(src, piece, t, direction):
        return pltpu.make_async_remote_copy(kv2.at[src, piece], kv2.at[src, piece], ring_s.at[t], ring_r.at[t],
                                            device_id=toward(direction))

    def send_own(direction, order):
        ring_copy(z, parity(c + order), 2 * order + direction, direction).start()

    def arrive(t):
        src, piece, direction = piece_of(t)
        ring_copy(src, piece, t, direction).wait_recv()
        last = 4 * (far - 1)

        @pl.when((t < last - 4) | (t == last - 4) | (t == last - 1))
        def _():
            ring_copy(src, piece, t + 4 - 2 * lax.div(t, last - 1), direction).start()

    def new_piece(u):
        dist = halve(u) + 1
        direction = parity(u)
        return lax.rem(z + dist * (2 * direction - 1) + nz, nz), direction

    def new_copy(src, u, direction):
        return pltpu.make_async_remote_copy(nk2.at[src], nk2.at[src], new_s.at[u], new_r.at[u], device_id=toward(direction))

    def attend(group, keys_values, causal=False):
        k_view, v_view = keys_values.at[0], keys_values.at[1]
        keys = k_view.shape[0]
        kb = min(256, keys)
        blocks = keys // kb

        def scores(h):
            top = None
            for b in range(blocks):
                s = product(k_view[b * kb:(b + 1) * kb], qb[group, h])
                if causal:
                    key = lax.broadcasted_iota(jnp.int32, s.shape, 0) + b * kb
                    query = lax.broadcasted_iota(jnp.int32, s.shape, 1)
                    s = jnp.where(key <= query, s, -jnp.inf)
                sbuf[h % 2, b * kb:(b + 1) * kb] = s
                part = jnp.max(s.reshape(kb // 8, 8, pair), axis=0)
                top = part if top is None else jnp.maximum(top, part)
            return top

        top = scores(0)
        for h in range(heads_dev):
            top_next = scores(h + 1) if h + 1 < heads_dev else None
            m_old = m_s[group, h]
            m_new = jnp.maximum(m_old, jnp.max(top, axis=0, keepdims=True))
            alpha = jnp.exp2((m_old - m_new) * score_mul)
            total = l_s[group, h] * alpha
            added = None
            for b in range(blocks):
                s = sbuf[h % 2, b * kb:(b + 1) * kb].reshape(kb // 8, 8, pair)
                p = jnp.exp2((s - m_new[None]) * score_mul)
                total = total + jnp.sum(p, axis=0)
                v_t = jnp.concatenate([v_view[b * kb + i * hd:b * kb + (i + 1) * hd] for i in range(kb // hd)], axis=1)
                part = product(v_t, p.reshape(kb, pair).astype(BF16))
                added = part if added is None else added + part
            acc[group, h] = (acc[group, h].reshape(hd // 8, 8, pair) * alpha[None]).reshape(hd, pair) + added
            l_s[group, h] = total
            m_s[group, h] = m_new
            top = top_next

    def new_arrive(u):
        src, direction = new_piece(u)
        new_copy(src, u, direction).wait_recv()

        @pl.when((u < n_new - 3) | (u == n_new - 3))
        def _():
            new_copy(src, u + 2, direction).start()

        @pl.when(src < z)
        def _():
            attend(0, nk2.at[src])

    def clear(groups):
        def one(i, carry):
            group, h = lax.div(i, heads_dev), lax.rem(i, heads_dev)
            m_s[group, h] = jnp.full(m_s.shape[2:], -jnp.inf, F32)
            l_s[group, h] = jnp.zeros(l_s.shape[2:], F32)
            acc[group, h] = jnp.zeros(acc.shape[2:], F32)
            return carry
        repeat(groups * heads_dev, one)

    def rope(vals):
        rounded = vals.astype(BF16).astype(F32)
        return rounded * cos_ref[...] + pltpu.roll(rounded, hd // 2, 1) * sin_ref[...]

    def rotation():
        base = base_rot[z]
        cos_ref[...] = base[0:1] * local_rot[0] - base[1:2] * local_rot[1]
        sin_ref[...] = base[3:4] * local_rot[0] + base[2:3] * local_rot[1]

    def project(layer):
        proj = product(xb[...], wqkv[...])
        q_bias, k_bias = (ref[...].astype(F32) for ref in ((bq1, bk1), (bq2, bk2))[layer])

        def bias_row(table, low, high):
            return jnp.where(c == 0, table[low:low + 1], table[high:high + 1])
        for h in range(heads_dev):
            cols = slice(h * hd, (h + 1) * hd)
            qb[0, h] = rope(proj[:, cols] + bias_row(q_bias, h, heads_dev + h)).T.astype(BF16)
        k_rot = rope(proj[:, half:half + hd] + bias_row(k_bias, 0, 1)).astype(BF16)
        own_new(layer)[0] = k_rot
        knew[layer] = k_rot
        v_val = proj[:, half + hd:]
        vnew[layer] = v_val.astype(BF16)
        for i in range(pair // hd):
            own_new(layer)[1, i * hd:(i + 1) * hd] = v_val[i * hd:(i + 1) * hd].T.astype(BF16)

    def append_swap(layer, j):
        return pltpu.make_async_remote_copy((knew, vnew)[j].at[layer, other_rows], app_in.at[layer, j],
                                            d2d_s.at[8 + 2 * layer + j], d2d_r.at[8 + 2 * layer + j], device_id={"cp": partner})

    def send_append(layer):
        for j in range(CORES):
            append_swap(layer, j).start()

    def put_append(layer):
        return pltpu.make_async_copy(app_buf.at[layer], app_out.at[layer], loc.at[9 + layer])

    def append(layer):
        for j in range(CORES):
            append_swap(layer, j).wait_recv()
            mine = (knew, vnew)[j][layer, own_rows].astype(F32)
            theirs = app_in[layer, j].astype(F32)
            wide[pl.ds(0, tok, stride=2)] = jnp.where(c == 0, mine, theirs)
            wide[pl.ds(1, tok, stride=2)] = jnp.where(c == 0, theirs, mine)
            app_buf[layer, j] = wide[pl.ds(0, 2 * tok)].astype(BF16)
        put_append(layer).start()

    def finish_heads(layer):
        for h in range(heads_dev):
            total = jnp.sum(l_s[0, h], axis=0, keepdims=True)
            summed = acc[0, h]
            if layer == 0:
                m_own, m_far = m_s[0, h, 0:1], far_ml[h:h + 1]
                m_all = jnp.maximum(m_own, m_far)
                w_own, w_far = jnp.exp2((m_own - m_all) * score_mul), jnp.exp2((m_far - m_all) * score_mul)
                total = total * w_own + far_ml[8 + h:9 + h] * w_far
                summed = summed * w_own + far_acc[h] * w_far
            ob[layer, c, :, h * hd:(h + 1) * hd] = (summed / total).T.astype(BF16)

    def hand_back():
        for h in range(heads_dev):
            part_ml[h:h + 1] = m_s[1, h, 0:1]
            part_ml[8 + h:9 + h] = jnp.sum(l_s[1, h], axis=0, keepdims=True)
        swap_acc.start()
        swap_ml.start()

    def attend_first():
        def step(k, carry):
            @pl.when(k == 2)
            def _():
                relay(1, 0, 5)
                relay(4, 0, 2)
                relay_new(1, 5)
                relay_new(4, 2)

            @pl.when(k == 3)
            def _():
                swap_q.wait_recv()

            @pl.when(k == 6)
            def _():
                relay(1, 1, 5)

            @pl.when(k == 8)
            def _():
                relay(4, 1, 2)
                pair_copy(2, 0).wait_recv()

            @pl.when(k == 10)
            def _():
                relay(5, 0, 3)
                pair_copy(2, 1).wait_recv()
                pair_new(2).wait_recv()
                relay_new(5, 3)

            @pl.when(k == 12)
            def _():
                relay(5, 1, 3)
                for direction in (odd, 1 - odd):
                    for order in range(CORES):
                        send_own(direction, order)

            @pl.when(k == 14)
            def _():
                pair_new(3).wait_recv()

            @pl.when((k == 12) | (k == 14))
            def _():
                turn = halve(k - 12)

                def new_step(i, carry):
                    slot, group = halve(i), parity(i)
                    src = lax.rem(z + nz + slot * (2 * odd - 1), nz)

                    @pl.when(src < (1 - group) * z + group * mate)
                    def _():
                        attend(group, nk1.at[slot])
                    return carry
                lax.fori_loop(6 * turn, 6 + 2 * turn, new_step, 0)

            @pl.when(k == 12)
            def _():
                pair_copy(3, 0).wait_recv()

            @pl.when(k == 14)
            def _():
                pair_copy(3, 1).wait_recv()

            @pl.when(k == 15)
            def _():
                hand_back()

            early = 1 - lax.div(k + 10, 16)
            i, end = lax.rem(k, 3), lax.div(k, 12)
            slot = early * halve(i) + (1 - early) * lax.div(k, 4)
            order = early * parity(i) + (1 - early) * lax.rem(halve(k), 2)
            group = early * lax.div(k, 3) + (1 - early) * (parity(k) * (1 - 2 * end) + end)
            piece = parity(c + order)
            attend(group, kv1.at[slot, piece])
            return carry

        repeat(16, step)

    def attend_second():
        def step(s, carry):
            @pl.when((s == 8) | (s == 9))
            def _():
                arrive(s)

            @pl.when(s >= 12)
            def _():
                arrive(s - 2)
            own = 1 - lax.div(s + n_steps - 2, n_steps)
            src, piece, _ = piece_of(lax.rem(s + n_steps - 2, n_steps))
            src = own * z + (1 - own) * src
            piece = own * parity(c + s) + (1 - own) * piece
            attend(0, kv2.at[src, piece])

            @pl.when((s == 7) | (s == 13) | (s == n_steps - 1))
            def _():
                last = lax.div(s, n_steps - 1)
                lo = (s - 11) * lax.div(s, 13)

                def new_step(u, carry):
                    new_arrive(u)
                    return carry
                lax.fori_loop(lo, lo + 2 + last, new_step, 0)
            return carry

        repeat(n_steps, step)

    def span(body, lo, hi):
        def step(i, carry):
            body(i)
            return carry
        lax.fori_loop(lo, hi, step, 0)

    for j in range(CORES):
        load_cache(0, j).start()
    load_x.start()
    for cpy in load_wqkv(0):
        cpy.start()
    barrier = pltpu.get_barrier_semaphore()
    for other in (partner, 2 * mate + c, 2 * near + c):
        pl.semaphore_signal(barrier, inc=1, device_id={"cp": other})
    for j in range(CORES):
        load_cache(0, j).wait()
    split_cache(0)
    pl.semaphore_wait(barrier, 3)
    for slot in (1, 4):
        pair_copy(slot, 0).start()
    swap_cache(0).start()
    swap_x.start()
    for j in range(CORES):
        load_cache(1, j).start()
    rotation()
    load_x.wait()
    swap_x.wait_recv()
    for cpy in load_wqkv(0):
        cpy.wait()
    project(0)
    for slot in (1, 4):
        pair_new(slot).start()
    swap_q.start()
    swap_cache(0).wait_recv()
    for slot in (1, 4):
        pair_copy(slot, 1).start()
    send_append(0)
    load_wo(0).start()
    for cpy in load_wqkv(1):
        cpy.start()
    for slot in range(W_SLOTS):
        for cpy in load_ff(slot, slot):
            cpy.start()
    clear(2)
    attend(0, nk1.at[0], causal=True)
    for j in range(CORES):
        load_cache(1, j).wait()
    split_cache(1)
    swap_cache(1).start()
    append(0)
    swap_cache(1).wait_recv()
    attend_first()
    span(arrive, 0, 2)
    swap_acc.wait_recv()
    swap_ml.wait_recv()
    finish_heads(0)

    swap_o = pltpu.make_async_remote_copy(ob.at[0, c], ob.at[0, c], d2d_s.at[5], d2d_r.at[5], device_id={"cp": partner})
    swap_o.start()
    load_wo(0).wait()
    swap_o.wait_recv()
    y_one = (product(ob[0, 0], wob[:half])
             + product(ob[0, 1], wob[half:])).astype(BF16)
    h_val = (xb[...].astype(F32) + y_one.astype(F32)).astype(BF16)
    hb[...] = h_val
    xb[...] = rms_norm(h_val.astype(F32))
    load_wo(1).start()
    gacc[...] = jnp.zeros(gacc.shape, F32)

    def ff_step(i, carry):
        slot = lax.rem(i, W_SLOTS)
        for cpy in load_ff(i, slot):
            cpy.wait()
        both = product(xb[...], w13[slot]).astype(BF16).astype(F32)
        gate = both[:, :FF_TILE]
        mixed = (gate * jax.nn.sigmoid(gate) * both[:, FF_TILE:]).astype(BF16)
        gacc[...] += product(mixed, w2b[slot])

        @pl.when(i == tiles - 2)
        def _():
            span(arrive, 4, 6)

        @pl.when(i + W_SLOTS < tiles)
        def _():
            for cpy in load_ff(i + W_SLOTS, slot):
                cpy.start()
        return carry

    span(arrive, 2, 4)
    repeat(tiles, ff_step)
    swap_g = pltpu.make_async_remote_copy(gacc, grecv, d2d_s.at[7], d2d_r.at[7], device_id={"cp": partner})
    swap_g.start()
    swap_g.wait_recv()
    g_val = (hb[...].astype(F32) + (gacc[...] + grecv[...])).astype(BF16)
    hb[...] = g_val
    put_g = pltpu.make_async_copy(hb.at[own_rows], g_out, loc.at[11])
    put_g.start()
    xb[...] = rms_norm(g_val.astype(F32))
    for cpy in load_wqkv(1):
        cpy.wait()
    swap_q.wait_send()
    project(1)
    for direction in range(CORES):
        new_copy(z, direction, direction).start()
    span(arrive, 6, 8)
    send_append(1)

    clear(1)
    attend(0, nk2.at[z], causal=True)
    append(1)
    attend_second()
    finish_heads(1)
    swap_y = pltpu.make_async_remote_copy(ob.at[1, c, other_rows], ob.at[1, c, other_rows], d2d_s.at[6], d2d_r.at[6],
                                          device_id={"cp": partner})
    swap_y.start()
    load_wo(1).wait()
    swap_y.wait_recv()
    ybuf[...] = (product(ob[1, 0, own_rows], wob[:half])
                 + product(ob[1, 1, own_rows], wob[half:])).astype(BF16)
    put_y = pltpu.make_async_copy(ybuf, y_out, loc.at[12])
    put_y.start()

    for layer in range(CORES):
        put_append(layer).wait()
        swap_cache(layer).wait_send()
        for j in range(CORES):
            append_swap(layer, j).wait_send()
    span(lambda t: ring_copy(0, 0, t, 0).wait_send(), 0, n_arr)
    span(lambda u: new_copy(0, u, 0).wait_send(), 0, n_new)
    for slot in range(1, 6):
        for order in range(CORES):
            pair_copy(slot, order).wait_send()
        pair_new(slot).wait_send()
    swap_acc.wait_send()
    swap_ml.wait_send()
    swap_x.wait_send()
    swap_o.wait_send()
    swap_g.wait_send()
    swap_y.wait_send()
    put_g.wait()
    put_y.wait()


def rotation_tables(n, tok, cache_dev, hd):
    half_dim = hd // 2
    inv_freq = np.tile(ROPE_THETA ** (-np.arange(half_dim) * (2.0 / hd)), 2)
    pair = CORES * tok
    offset = np.arange(pair)[:, None] * inv_freq[None, :]
    base = (n * cache_dev + np.arange(n // 2) * pair)[:, None] * inv_freq[None, :]
    sign = np.where(np.arange(hd) < half_dim, -1.0, 1.0)[None, :]
    local_rot = np.stack([np.cos(offset), np.sin(offset)])
    base_rot = np.stack([np.cos(base), np.sin(base), sign * np.cos(base), sign * np.sin(base)], axis=1)
    return jnp.asarray(local_rot, F32), jnp.asarray(base_rot, F32)


def copy_kernel(g_in, y_in, app_in, g_out, y_out, *rest):
    app_outs, (g_buf, y_buf, app_buf, sems) = rest[:4], rest[4:]
    ins = [pltpu.make_async_copy(src, buf, sems.at[0, i]) for i, (src, buf) in enumerate(((y_in, y_buf), (g_in, g_buf), (app_in, app_buf)))]
    outs = [[pltpu.make_async_copy(y_buf, y_out, sems.at[1, 0])], [pltpu.make_async_copy(g_buf, g_out, sems.at[1, 1])],
            [pltpu.make_async_copy(app_buf.at[i // 2, i % 2], app_outs[i], sems.at[1, 2 + i]) for i in range(4)]]
    for cpy in ins:
        cpy.start()
    for cpy, group in zip(ins, outs):
        cpy.wait()
        for out in group:
            out.start()
    for group in outs:
        for out in group:
            out.wait()


def hand_over(hidden, y_two, app):
    any_spec = pl.BlockSpec(memory_space=pl.ANY)
    row_shape = jax.ShapeDtypeStruct(hidden.shape, hidden.dtype)
    app_shape = jax.ShapeDtypeStruct(app.shape[2:], app.dtype)
    return pl.pallas_call(
        copy_kernel,
        out_shape=[row_shape, row_shape] + [app_shape] * 4,
        in_specs=[any_spec] * 3,
        out_specs=[any_spec] * 6,
        scratch_shapes=[pltpu.VMEM(hidden.shape, BF16), pltpu.VMEM(hidden.shape, BF16), pltpu.VMEM(app.shape, BF16),
                        pltpu.SemaphoreType.DMA((2, 6))],
        name="hand_over",
    )(hidden, y_two, app)


def fused_blocks(n, x_in, cache, weights, biases, tables):
    tok, d_model = x_in.shape
    cache_dev, kv_heads, hd = cache[0].shape
    w_q1, w_gate = weights[0], weights[4]
    heads_dev = w_q1.shape[1] // hd // kv_heads
    half = heads_dev * hd
    nz = n // CORES
    far = nz // CORES
    n_arr = 4 * (far - 1) + 2
    n_new = 2 * (far - 1) + 1
    pair = CORES * tok
    rows = [arr.reshape(cache_dev * kv_heads, hd) for arr in cache]
    any_spec = pl.BlockSpec(memory_space=pl.ANY)
    vmem_spec = pl.BlockSpec(memory_space=pltpu.VMEM)
    dma = pltpu.SemaphoreType.DMA
    ff_half = w_gate.shape[1] // 2
    flops = 2 * pair * (d_model * (half + 2 * hd) * 2 + 3 * d_model * ff_half + 2 * half * d_model * 2) + 8 * pair * half * n * cache_dev
    return pl.pallas_call(
        functools.partial(block_kernel, n),
        out_shape=(jax.ShapeDtypeStruct((tok, d_model), BF16), jax.ShapeDtypeStruct((tok, d_model), BF16),
                   jax.ShapeDtypeStruct((2, 2, kv_heads * tok, hd), BF16)),
        in_specs=[any_spec] * 16 + [vmem_spec] * 6,
        out_specs=(any_spec, any_spec, any_spec),
        scratch_shapes=[
            pltpu.VMEM((6, 2, 2, cache_dev, hd), BF16),
            pltpu.VMEM((nz, 2, 2, cache_dev, hd), BF16),
            pltpu.VMEM((6, 2, pair, hd), BF16),
            pltpu.VMEM((nz, 2, pair, hd), BF16),
            pltpu.VMEM((16, pair), F32),
            pltpu.VMEM((heads_dev, hd, pair), F32),
            pltpu.VMEM((16, pair), F32),
            pltpu.VMEM((CORES, CORES, 2 * cache_dev, hd), BF16),
            pltpu.VMEM((CORES, CORES, cache_dev, hd), BF16),
            pltpu.VMEM((2 * hd, hd), F32),
            pltpu.VMEM((CORES, cache_dev, pair), F32),
            pltpu.VMEM((pair, hd), F32),
            pltpu.VMEM((pair, hd), F32),
            pltpu.VMEM((CORES, pair, hd), BF16),
            pltpu.VMEM((CORES, pair, hd), BF16),
            pltpu.VMEM((CORES, CORES, tok, hd), BF16),
            pltpu.VMEM((CORES, CORES, pair, hd), BF16),
            pltpu.VMEM((pair, d_model), BF16),
            pltpu.VMEM((pair, d_model), BF16),
            pltpu.VMEM((CORES, heads_dev, hd, pair), BF16),
            pltpu.VMEM((CORES, heads_dev, hd, pair), F32),
            pltpu.VMEM((CORES, heads_dev, 8, pair), F32),
            pltpu.VMEM((CORES, heads_dev, 8, pair), F32),
            pltpu.VMEM((CORES, CORES, pair, half), BF16),
            pltpu.VMEM((pair, d_model), F32),
            pltpu.VMEM((pair, d_model), F32),
            pltpu.VMEM((tok, d_model), BF16),
            pltpu.VMEM((d_model, half + 2 * hd), BF16),
            pltpu.VMEM((2 * half, d_model), BF16),
            pltpu.VMEM((W_SLOTS, d_model, 2 * FF_TILE), BF16),
            pltpu.VMEM((W_SLOTS, FF_TILE, d_model), BF16),
            dma((6, 3)), dma((6, 3)), dma((n_arr,)), dma((n_arr,)), dma((n_new,)), dma((n_new,)),
            dma((12,)), dma((12,)), dma((13,)), dma((W_SLOTS, 3)),
        ],
        compiler_params=pltpu.CompilerParams(collective_id=0, has_side_effects=True, vmem_limit_bytes=67043328),
        cost_estimate=pl.CostEstimate(flops=flops, bytes_accessed=6 * d_model * ff_half, transcendentals=0),
        name="fused_blocks",
    )(x_in, *rows, *weights, *biases, *tables)


def solution(mesh):
    axis_size = mesh.shape['cp']
    rows_spec = P(('dp', 'cp'), None)
    cache_spec = P(('dp', 'cp'), None, None)
    mat_spec = P(None, None)
    vec_spec = P(None)
    layer_specs = (cache_spec, cache_spec, mat_spec, vec_spec, mat_spec, vec_spec, mat_spec, mat_spec)
    in_specs = (rows_spec,) + layer_specs + (mat_spec, mat_spec, mat_spec) + layer_specs
    out_specs = (rows_spec, rows_spec, cache_spec, cache_spec, cache_spec, cache_spec)

    def forward(x_in, cache_k1, cache_v1, w_q1, b_q1, w_k1, b_k1, w_v1, w_o1, w_gate, w_up, w_down, cache_k2, cache_v2, w_q2, b_q2, w_k2, b_k2, w_v2, w_o2):
        tok = x_in.shape[0]
        cache_dev, kv_heads, hd = cache_k1.shape
        tables = rotation_tables(axis_size, tok, cache_dev, hd)
        biases = [part.reshape(-1, hd) for part in (b_q1, b_k1, b_q2, b_k2)]
        weights = (w_q1, w_k1, w_v1, w_o1, w_gate, w_up, w_down, w_q2, w_k2, w_v2, w_o2)
        hidden, y_two, app = fused_blocks(axis_size, x_in, (cache_k1, cache_v1, cache_k2, cache_v2), weights, biases, tables)
        outs = hand_over(hidden, y_two, app)
        return (outs[0], outs[1], *(arr.reshape(tok, kv_heads, hd) for arr in outs[2:]))

    return jax.shard_map(forward, mesh=mesh, in_specs=in_specs, out_specs=out_specs, check_vma=False)
```

```python
import functools

import jax
import jax.numpy as jnp
import numpy as np
from jax import lax
from jax.experimental import pallas as pl
from jax.experimental.pallas import tpu as pltpu
from jax.sharding import PartitionSpec as P

ROPE_THETA = 500000.0
NORM_EPS = 1e-5
LOG2E = 1.4426950408889634
BF16 = jnp.bfloat16
F32 = jnp.float32
FF_TILE = 640
W_SLOTS = 3
CORES = 2


def parity(i):
    return lax.rem(i, CORES)


def halve(i):
    return lax.div(i, CORES)


def repeat(count, body):
    lax.fori_loop(0, count, body, 0)


def product(left, right):
    return jnp.dot(left, right, preferred_element_type=F32)


def rms_norm(wide):
    return (wide * lax.rsqrt(jnp.mean(wide * wide, axis=-1, keepdims=True) + NORM_EPS)).astype(BF16)


def block_kernel(n, x_ref, kc1, vc1, kc2, vc2, wq1, wk1, wv1, wo1, wg, wu, wd, wq2, wk2, wv2, wo2, bq1, bk1, bq2, bk2, local_rot, base_rot,
                 g_out, y_out, app_out,
                 kv1, kv2, nk1, nk2, part_ml, far_acc, far_ml, raw, snd, wide, sbuf, cos_ref, sin_ref, knew, vnew, app_in, app_buf,
                 xb, hb, qb, acc, m_s, l_s, ob, gacc, grecv, ybuf, wqkv, wob, w13, w2b,
                 pair_s, pair_r, ring_s, ring_r, new_s, new_r, d2d_s, d2d_r, loc, wsem):
    nz = n // CORES
    far = nz // CORES
    n_arr = 4 * (far - 1) + 2
    n_new = 2 * (far - 1) + 1
    cp = lax.axis_index("cp")
    c = parity(cp)
    z = halve(cp)
    partner = cp + 1 - 2 * c
    odd = parity(z)
    mate = z + 1 - 2 * odd
    near = lax.rem(z + nz - 1 + 2 * odd, nz)
    tok = x_ref.shape[0]
    heads_dev = qb.shape[1]
    hd = qb.shape[2]
    pair = CORES * tok
    cache_dev = kv1.shape[3]
    n_steps = n_arr + 2
    half = heads_dev * hd
    ff_half = wg.shape[1] // 2
    tiles = ff_half // FF_TILE
    cache = (kc1, vc1), (kc2, vc2)
    wqkv_src = (wq1, wk1, wv1), (wq2, wk2, wv2)
    wo_src = (wo1, wo2)
    score_mul = hd ** -0.5 * LOG2E

    def toward(direction):
        return {"cp": lax.rem(cp + n + 2 - 4 * direction, n)}

    def chip(index):
        return {"cp": 2 * index + c}

    def own_slot(layer):
        return kv1.at[0] if layer == 0 else kv2.at[z]

    def own_new(layer):
        return nk1.at[0] if layer == 0 else nk2.at[z]

    def load_cache(layer, j):
        return pltpu.make_async_copy(cache[layer][j], raw.at[layer, j], loc.at[1 + 2 * layer + j])

    def swap_cache(layer):
        return pltpu.make_async_remote_copy(snd.at[layer], own_slot(layer).at[c], d2d_s.at[1 + layer], d2d_r.at[1 + layer],
                                            device_id={"cp": partner})

    def split_cache(layer):
        for j in range(CORES):
            def one_block(b, carry):
                wide[...] = raw[layer, j, pl.ds(pl.multiple_of(b * 2 * hd, 2 * hd), 2 * hd)].astype(F32)
                first = wide[pl.ds(0, hd, stride=2)]
                second = wide[pl.ds(1, hd, stride=2)]
                mine = jnp.where(c == 0, first, second)
                theirs = jnp.where(c == 0, second, first)
                if j == 1:
                    mine, theirs = mine.T, theirs.T
                rows = pl.ds(pl.multiple_of(b * hd, hd), hd)
                own_slot(layer)[c, j, rows] = mine.astype(BF16)
                snd[layer, j, rows] = theirs.astype(BF16)
                return carry
            repeat(cache_dev // hd, one_block)

    own_rows = pl.ds(pl.multiple_of(c * tok, tok), tok)
    other_rows = pl.ds(pl.multiple_of((1 - c) * tok, tok), tok)
    load_x = pltpu.make_async_copy(x_ref, xb.at[own_rows], loc.at[0])
    swap_x = pltpu.make_async_remote_copy(x_ref, xb.at[own_rows], d2d_s.at[0], d2d_r.at[0], device_id={"cp": partner})

    def load_wqkv(layer):
        w_q, w_k, w_v = wqkv_src[layer]
        return (pltpu.make_async_copy(w_q.at[:, pl.ds(pl.multiple_of(c * half, hd), half)], wqkv.at[:, pl.ds(0, half)], loc.at[5]),
                pltpu.make_async_copy(w_k.at[:, pl.ds(pl.multiple_of(c * hd, hd), hd)], wqkv.at[:, pl.ds(half, hd)], loc.at[6]),
                pltpu.make_async_copy(w_v.at[:, pl.ds(pl.multiple_of(c * hd, hd), hd)], wqkv.at[:, pl.ds(half + hd, hd)], loc.at[7]))

    def load_wo(layer):
        return pltpu.make_async_copy(wo_src[layer], wob, loc.at[8])

    def load_ff(tile, slot):
        cols = pl.ds(pl.multiple_of(c * ff_half + tile * FF_TILE, 128), FF_TILE)
        return (pltpu.make_async_copy(wg.at[:, cols], w13.at[slot, :, pl.ds(0, FF_TILE)], wsem.at[slot, 0]),
                pltpu.make_async_copy(wu.at[:, cols], w13.at[slot, :, pl.ds(FF_TILE, FF_TILE)], wsem.at[slot, 1]),
                pltpu.make_async_copy(wd.at[cols], w2b.at[slot], wsem.at[slot, 2]))


    hops = (None, (0, near), (4, near), (5, near), (0, mate), (1, mate))

    def pair_copy(slot, order):
        src, target = hops[slot]
        piece = parity(c + order)
        return pltpu.make_async_remote_copy(kv1.at[src, piece], kv1.at[slot, piece], pair_s.at[slot, order],
                                            pair_r.at[slot, order], device_id=chip(target))

    def pair_new(slot):
        src, target = hops[slot]
        return pltpu.make_async_remote_copy(nk1.at[src], nk1.at[slot], pair_s.at[slot, 2], pair_r.at[slot, 2], device_id=chip(target))

    def relay(slot, order, onto):
        pair_copy(slot, order).wait_recv()
        pair_copy(onto, order).start()

    def relay_new(slot, onto):
        pair_new(slot).wait_recv()
        pair_new(onto).start()

    swap_q = pltpu.make_async_remote_copy(qb.at[0], qb.at[1], pair_s.at[0, 0], pair_r.at[0, 0], device_id=chip(mate))
    swap_acc = pltpu.make_async_remote_copy(acc.at[1], far_acc, pair_s.at[0, 1], pair_r.at[0, 1], device_id=chip(mate))
    swap_ml = pltpu.make_async_remote_copy(part_ml, far_ml, pair_s.at[0, 2], pair_r.at[0, 2], device_id=chip(mate))

    def piece_of(t):
        dist = lax.div(t, 4) + 1
        r = lax.rem(t, 4)
        direction = parity(t)
        order = halve(r) + parity(r) * lax.div(dist, far)
        src = lax.rem(z + nz + dist * (2 * direction - 1), nz)
        return src, parity(c + order), direction

    def ring_copy(src, piece, t, direction):
        return pltpu.make_async_remote_copy(kv2.at[src, piece], kv2.at[src, piece], ring_s.at[t], ring_r.at[t],
                                            device_id=toward(direction))

    def send_own(direction, order):
        ring_copy(z, parity(c + order), 2 * order + direction, direction).start()

    def arrive(t):
        src, piece, direction = piece_of(t)
        ring_copy(src, piece, t, direction).wait_recv()
        last = 4 * (far - 1)

        @pl.when((t < last - 4) | (t == last - 4) | (t == last - 1))
        def _():
            ring_copy(src, piece, t + 4 - 2 * lax.div(t, last - 1), direction).start()

    def new_piece(u):
        dist = halve(u) + 1
        direction = parity(u)
        return lax.rem(z + dist * (2 * direction - 1) + nz, nz), direction

    def new_copy(src, u, direction):
        return pltpu.make_async_remote_copy(nk2.at[src], nk2.at[src], new_s.at[u], new_r.at[u], device_id=toward(direction))

    def attend(group, keys_values, causal=False):
        k_view, v_view = keys_values.at[0], keys_values.at[1]
        keys = k_view.shape[0]
        kb = min(256, keys)
        blocks = keys // kb

        def scores(h):
            top = None
            for b in range(blocks):
                s = product(k_view[b * kb:(b + 1) * kb], qb[group, h])
                if causal:
                    key = lax.broadcasted_iota(jnp.int32, s.shape, 0) + b * kb
                    query = lax.broadcasted_iota(jnp.int32, s.shape, 1)
                    s = jnp.where(key <= query, s, -jnp.inf)
                sbuf[h % 2, b * kb:(b + 1) * kb] = s
                part = jnp.max(s.reshape(kb // 8, 8, pair), axis=0)
                top = part if top is None else jnp.maximum(top, part)
            return top

        top = scores(0)
        for h in range(heads_dev):
            top_next = scores(h + 1) if h + 1 < heads_dev else None
            m_old = m_s[group, h]
            m_new = jnp.maximum(m_old, jnp.max(top, axis=0, keepdims=True))
            alpha = jnp.exp2((m_old - m_new) * score_mul)
            total = l_s[group, h] * alpha
            added = None
            for b in range(blocks):
                s = sbuf[h % 2, b * kb:(b + 1) * kb].reshape(kb // 8, 8, pair)
                p = jnp.exp2((s - m_new[None]) * score_mul)
                total = total + jnp.sum(p, axis=0)
                v_t = jnp.concatenate([v_view[b * kb + i * hd:b * kb + (i + 1) * hd] for i in range(kb // hd)], axis=1)
                part = product(v_t, p.reshape(kb, pair).astype(BF16))
                added = part if added is None else added + part
            acc[group, h] = (acc[group, h].reshape(hd // 8, 8, pair) * alpha[None]).reshape(hd, pair) + added
            l_s[group, h] = total
            m_s[group, h] = m_new
            top = top_next

    def new_arrive(u):
        src, direction = new_piece(u)
        new_copy(src, u, direction).wait_recv()

        @pl.when((u < n_new - 3) | (u == n_new - 3))
        def _():
            new_copy(src, u + 2, direction).start()

        @pl.when(src < z)
        def _():
            attend(0, nk2.at[src])

    def clear(groups):
        def one(i, carry):
            group, h = lax.div(i, heads_dev), lax.rem(i, heads_dev)
            m_s[group, h] = jnp.full(m_s.shape[2:], -jnp.inf, F32)
            l_s[group, h] = jnp.zeros(l_s.shape[2:], F32)
            acc[group, h] = jnp.zeros(acc.shape[2:], F32)
            return carry
        repeat(groups * heads_dev, one)

    def rope(vals):
        rounded = vals.astype(BF16).astype(F32)
        return rounded * cos_ref[...] + pltpu.roll(rounded, hd // 2, 1) * sin_ref[...]

    def rotation():
        base = base_rot[z]
        cos_ref[...] = base[0:1] * local_rot[0] - base[1:2] * local_rot[1]
        sin_ref[...] = base[3:4] * local_rot[0] + base[2:3] * local_rot[1]

    def project(layer):
        proj = product(xb[...], wqkv[...])
        q_bias, k_bias = (ref[...].astype(F32) for ref in ((bq1, bk1), (bq2, bk2))[layer])

        def bias_row(table, low, high):
            return jnp.where(c == 0, table[low:low + 1], table[high:high + 1])
        for h in range(heads_dev):
            cols = slice(h * hd, (h + 1) * hd)
            qb[0, h] = rope(proj[:, cols] + bias_row(q_bias, h, heads_dev + h)).T.astype(BF16)
        k_rot = rope(proj[:, half:half + hd] + bias_row(k_bias, 0, 1)).astype(BF16)
        own_new(layer)[0] = k_rot
        knew[layer] = k_rot
        v_val = proj[:, half + hd:]
        vnew[layer] = v_val.astype(BF16)
        for i in range(pair // hd):
            own_new(layer)[1, i * hd:(i + 1) * hd] = v_val[i * hd:(i + 1) * hd].T.astype(BF16)

    def append_swap(layer, j):
        return pltpu.make_async_remote_copy((knew, vnew)[j].at[layer, other_rows], app_in.at[layer, j],
                                            d2d_s.at[8 + 2 * layer + j], d2d_r.at[8 + 2 * layer + j], device_id={"cp": partner})

    def send_append(layer):
        for j in range(CORES):
            append_swap(layer, j).start()

    def put_append(layer):
        return pltpu.make_async_copy(app_buf.at[layer], app_out.at[layer], loc.at[9 + layer])

    def append(layer):
        for j in range(CORES):
            append_swap(layer, j).wait_recv()
            mine = (knew, vnew)[j][layer, own_rows].astype(F32)
            theirs = app_in[layer, j].astype(F32)
            wide[pl.ds(0, tok, stride=2)] = jnp.where(c == 0, mine, theirs)
            wide[pl.ds(1, tok, stride=2)] = jnp.where(c == 0, theirs, mine)
            app_buf[layer, j] = wide[pl.ds(0, 2 * tok)].astype(BF16)
        put_append(layer).start()

    def finish_heads(layer):
        for h in range(heads_dev):
            total = jnp.sum(l_s[0, h], axis=0, keepdims=True)
            summed = acc[0, h]
            if layer == 0:
                m_own, m_far = m_s[0, h, 0:1], far_ml[h:h + 1]
                m_all = jnp.maximum(m_own, m_far)
                w_own, w_far = jnp.exp2((m_own - m_all) * score_mul), jnp.exp2((m_far - m_all) * score_mul)
                total = total * w_own + far_ml[8 + h:9 + h] * w_far
                summed = summed * w_own + far_acc[h] * w_far
            ob[layer, c, :, h * hd:(h + 1) * hd] = (summed / total).T.astype(BF16)

    def hand_back():
        for h in range(heads_dev):
            part_ml[h:h + 1] = m_s[1, h, 0:1]
            part_ml[8 + h:9 + h] = jnp.sum(l_s[1, h], axis=0, keepdims=True)
        swap_acc.start()
        swap_ml.start()

    def attend_first():
        def step(k, carry):
            @pl.when(k == 2)
            def _():
                relay(1, 0, 5)
                relay(4, 0, 2)
                relay_new(1, 5)
                relay_new(4, 2)

            @pl.when(k == 3)
            def _():
                swap_q.wait_recv()

            @pl.when(k == 6)
            def _():
                relay(1, 1, 5)

            @pl.when(k == 8)
            def _():
                relay(4, 1, 2)
                pair_copy(2, 0).wait_recv()

            @pl.when(k == 10)
            def _():
                relay(5, 0, 3)
                pair_copy(2, 1).wait_recv()
                pair_new(2).wait_recv()
                relay_new(5, 3)

            @pl.when(k == 12)
            def _():
                relay(5, 1, 3)
                for direction in (odd, 1 - odd):
                    for order in range(CORES):
                        send_own(direction, order)

            @pl.when(k == 14)
            def _():
                pair_new(3).wait_recv()

            @pl.when((k == 12) | (k == 14))
            def _():
                turn = halve(k - 12)

                def new_step(i, carry):
                    slot, group = halve(i), parity(i)
                    src = lax.rem(z + nz + slot * (2 * odd - 1), nz)

                    @pl.when(src < (1 - group) * z + group * mate)
                    def _():
                        attend(group, nk1.at[slot])
                    return carry
                lax.fori_loop(6 * turn, 6 + 2 * turn, new_step, 0)

            @pl.when(k == 12)
            def _():
                pair_copy(3, 0).wait_recv()

            @pl.when(k == 14)
            def _():
                pair_copy(3, 1).wait_recv()

            @pl.when(k == 15)
            def _():
                hand_back()

            early = 1 - lax.div(k + 10, 16)
            i, end = lax.rem(k, 3), lax.div(k, 12)
            slot = early * halve(i) + (1 - early) * lax.div(k, 4)
            order = early * parity(i) + (1 - early) * lax.rem(halve(k), 2)
            group = early * lax.div(k, 3) + (1 - early) * (parity(k) * (1 - 2 * end) + end)
            piece = parity(c + order)
            attend(group, kv1.at[slot, piece])
            return carry

        repeat(16, step)

    def attend_second():
        def step(s, carry):
            @pl.when((s == 8) | (s == 9))
            def _():
                arrive(s)

            @pl.when(s >= 12)
            def _():
                arrive(s - 2)
            own = 1 - lax.div(s + n_steps - 2, n_steps)
            src, piece, _ = piece_of(lax.rem(s + n_steps - 2, n_steps))
            src = own * z + (1 - own) * src
            piece = own * parity(c + s) + (1 - own) * piece
            attend(0, kv2.at[src, piece])

            @pl.when((s == 7) | (s == 11) | (s == n_steps - 1))
            def _():
                last = lax.div(s, n_steps - 1)
                lo = halve(s - 7)

                def new_step(u, carry):
                    new_arrive(u)
                    return carry
                lax.fori_loop(lo, lo + 2 + last, new_step, 0)
            return carry

        repeat(n_steps, step)

    def span(body, lo, hi):
        def step(i, carry):
            body(i)
            return carry
        lax.fori_loop(lo, hi, step, 0)

    for j in range(CORES):
        load_cache(0, j).start()
    load_x.start()
    for cpy in load_wqkv(0):
        cpy.start()
    barrier = pltpu.get_barrier_semaphore()
    for other in (partner, 2 * mate + c, 2 * near + c):
        pl.semaphore_signal(barrier, inc=1, device_id={"cp": other})
    for j in range(CORES):
        load_cache(0, j).wait()
    split_cache(0)
    pl.semaphore_wait(barrier, 3)
    for slot in (1, 4):
        pair_copy(slot, 0).start()
    swap_cache(0).start()
    swap_x.start()
    for j in range(CORES):
        load_cache(1, j).start()
    rotation()
    load_x.wait()
    swap_x.wait_recv()
    for cpy in load_wqkv(0):
        cpy.wait()
    project(0)
    for slot in (1, 4):
        pair_new(slot).start()
    swap_q.start()
    swap_cache(0).wait_recv()
    for slot in (1, 4):
        pair_copy(slot, 1).start()
    send_append(0)
    load_wo(0).start()
    for cpy in load_wqkv(1):
        cpy.start()
    for slot in range(W_SLOTS):
        for cpy in load_ff(slot, slot):
            cpy.start()
    clear(2)
    attend(0, nk1.at[0], causal=True)
    for j in range(CORES):
        load_cache(1, j).wait()
    split_cache(1)
    swap_cache(1).start()
    append(0)
    swap_cache(1).wait_recv()
    attend_first()
    span(arrive, 0, 2)
    swap_acc.wait_recv()
    swap_ml.wait_recv()
    finish_heads(0)

    swap_o = pltpu.make_async_remote_copy(ob.at[0, c], ob.at[0, c], d2d_s.at[5], d2d_r.at[5], device_id={"cp": partner})
    swap_o.start()
    load_wo(0).wait()
    swap_o.wait_recv()
    y_one = (product(ob[0, 0], wob[:half])
             + product(ob[0, 1], wob[half:])).astype(BF16)
    h_val = (xb[...].astype(F32) + y_one.astype(F32)).astype(BF16)
    hb[...] = h_val
    xb[...] = rms_norm(h_val.astype(F32))
    load_wo(1).start()
    gacc[...] = jnp.zeros(gacc.shape, F32)

    def ff_step(i, carry):
        slot = lax.rem(i, W_SLOTS)
        for cpy in load_ff(i, slot):
            cpy.wait()
        both = product(xb[...], w13[slot]).astype(BF16).astype(F32)
        gate = both[:, :FF_TILE]
        mixed = (gate * jax.nn.sigmoid(gate) * both[:, FF_TILE:]).astype(BF16)
        gacc[...] += product(mixed, w2b[slot])

        @pl.when(i == tiles - 2)
        def _():
            span(arrive, 4, 6)

        @pl.when(i + W_SLOTS < tiles)
        def _():
            for cpy in load_ff(i + W_SLOTS, slot):
                cpy.start()
        return carry

    span(arrive, 2, 4)
    repeat(tiles, ff_step)
    swap_g = pltpu.make_async_remote_copy(gacc, grecv, d2d_s.at[7], d2d_r.at[7], device_id={"cp": partner})
    swap_g.start()
    swap_g.wait_recv()
    g_val = (hb[...].astype(F32) + (gacc[...] + grecv[...])).astype(BF16)
    hb[...] = g_val
    put_g = pltpu.make_async_copy(hb.at[own_rows], g_out, loc.at[11])
    put_g.start()
    xb[...] = rms_norm(g_val.astype(F32))
    for cpy in load_wqkv(1):
        cpy.wait()
    swap_q.wait_send()
    project(1)
    for direction in range(CORES):
        new_copy(z, direction, direction).start()
    span(arrive, 6, 8)
    send_append(1)

    clear(1)
    attend(0, nk2.at[z], causal=True)
    append(1)
    attend_second()
    finish_heads(1)
    swap_y = pltpu.make_async_remote_copy(ob.at[1, c, other_rows], ob.at[1, c, other_rows], d2d_s.at[6], d2d_r.at[6],
                                          device_id={"cp": partner})
    swap_y.start()
    load_wo(1).wait()
    swap_y.wait_recv()
    ybuf[...] = (product(ob[1, 0, own_rows], wob[:half])
                 + product(ob[1, 1, own_rows], wob[half:])).astype(BF16)
    put_y = pltpu.make_async_copy(ybuf, y_out, loc.at[12])
    put_y.start()

    for layer in range(CORES):
        put_append(layer).wait()
        swap_cache(layer).wait_send()
        for j in range(CORES):
            append_swap(layer, j).wait_send()
    span(lambda t: ring_copy(0, 0, t, 0).wait_send(), 0, n_arr)
    span(lambda u: new_copy(0, u, 0).wait_send(), 0, n_new)
    for slot in range(1, 6):
        for order in range(CORES):
            pair_copy(slot, order).wait_send()
        pair_new(slot).wait_send()
    swap_acc.wait_send()
    swap_ml.wait_send()
    swap_x.wait_send()
    swap_o.wait_send()
    swap_g.wait_send()
    swap_y.wait_send()
    put_g.wait()
    put_y.wait()


def rotation_tables(n, tok, cache_dev, hd):
    half_dim = hd // 2
    inv_freq = np.tile(ROPE_THETA ** (-np.arange(half_dim) * (2.0 / hd)), 2)
    pair = CORES * tok
    offset = np.arange(pair)[:, None] * inv_freq[None, :]
    base = (n * cache_dev + np.arange(n // 2) * pair)[:, None] * inv_freq[None, :]
    sign = np.where(np.arange(hd) < half_dim, -1.0, 1.0)[None, :]
    local_rot = np.stack([np.cos(offset), np.sin(offset)])
    base_rot = np.stack([np.cos(base), np.sin(base), sign * np.cos(base), sign * np.sin(base)], axis=1)
    return jnp.asarray(local_rot, F32), jnp.asarray(base_rot, F32)


def copy_kernel(g_in, y_in, app_in, g_out, y_out, *rest):
    app_outs, (g_buf, y_buf, app_buf, sems) = rest[:4], rest[4:]
    ins = [pltpu.make_async_copy(src, buf, sems.at[0, i]) for i, (src, buf) in enumerate(((y_in, y_buf), (g_in, g_buf), (app_in, app_buf)))]
    outs = [[pltpu.make_async_copy(y_buf, y_out, sems.at[1, 0])], [pltpu.make_async_copy(g_buf, g_out, sems.at[1, 1])],
            [pltpu.make_async_copy(app_buf.at[i // 2, i % 2], app_outs[i], sems.at[1, 2 + i]) for i in range(4)]]
    for cpy in ins:
        cpy.start()
    for cpy, group in zip(ins, outs):
        cpy.wait()
        for out in group:
            out.start()
    for group in outs:
        for out in group:
            out.wait()


def hand_over(hidden, y_two, app):
    any_spec = pl.BlockSpec(memory_space=pl.ANY)
    row_shape = jax.ShapeDtypeStruct(hidden.shape, hidden.dtype)
    app_shape = jax.ShapeDtypeStruct(app.shape[2:], app.dtype)
    return pl.pallas_call(
        copy_kernel,
        out_shape=[row_shape, row_shape] + [app_shape] * 4,
        in_specs=[any_spec] * 3,
        out_specs=[any_spec] * 6,
        scratch_shapes=[pltpu.VMEM(hidden.shape, BF16), pltpu.VMEM(hidden.shape, BF16), pltpu.VMEM(app.shape, BF16),
                        pltpu.SemaphoreType.DMA((2, 6))],
        name="hand_over",
    )(hidden, y_two, app)


def fused_blocks(n, x_in, cache, weights, biases, tables):
    tok, d_model = x_in.shape
    cache_dev, kv_heads, hd = cache[0].shape
    w_q1, w_gate = weights[0], weights[4]
    heads_dev = w_q1.shape[1] // hd // kv_heads
    half = heads_dev * hd
    nz = n // CORES
    far = nz // CORES
    n_arr = 4 * (far - 1) + 2
    n_new = 2 * (far - 1) + 1
    pair = CORES * tok
    rows = [arr.reshape(cache_dev * kv_heads, hd) for arr in cache]
    any_spec = pl.BlockSpec(memory_space=pl.ANY)
    vmem_spec = pl.BlockSpec(memory_space=pltpu.VMEM)
    dma = pltpu.SemaphoreType.DMA
    ff_half = w_gate.shape[1] // 2
    flops = 2 * pair * (d_model * (half + 2 * hd) * 2 + 3 * d_model * ff_half + 2 * half * d_model * 2) + 8 * pair * half * n * cache_dev
    return pl.pallas_call(
        functools.partial(block_kernel, n),
        out_shape=(jax.ShapeDtypeStruct((tok, d_model), BF16), jax.ShapeDtypeStruct((tok, d_model), BF16),
                   jax.ShapeDtypeStruct((2, 2, kv_heads * tok, hd), BF16)),
        in_specs=[any_spec] * 16 + [vmem_spec] * 6,
        out_specs=(any_spec, any_spec, any_spec),
        scratch_shapes=[
            pltpu.VMEM((6, 2, 2, cache_dev, hd), BF16),
            pltpu.VMEM((nz, 2, 2, cache_dev, hd), BF16),
            pltpu.VMEM((6, 2, pair, hd), BF16),
            pltpu.VMEM((nz, 2, pair, hd), BF16),
            pltpu.VMEM((16, pair), F32),
            pltpu.VMEM((heads_dev, hd, pair), F32),
            pltpu.VMEM((16, pair), F32),
            pltpu.VMEM((CORES, CORES, 2 * cache_dev, hd), BF16),
            pltpu.VMEM((CORES, CORES, cache_dev, hd), BF16),
            pltpu.VMEM((2 * hd, hd), F32),
            pltpu.VMEM((CORES, cache_dev, pair), F32),
            pltpu.VMEM((pair, hd), F32),
            pltpu.VMEM((pair, hd), F32),
            pltpu.VMEM((CORES, pair, hd), BF16),
            pltpu.VMEM((CORES, pair, hd), BF16),
            pltpu.VMEM((CORES, CORES, tok, hd), BF16),
            pltpu.VMEM((CORES, CORES, pair, hd), BF16),
            pltpu.VMEM((pair, d_model), BF16),
            pltpu.VMEM((pair, d_model), BF16),
            pltpu.VMEM((CORES, heads_dev, hd, pair), BF16),
            pltpu.VMEM((CORES, heads_dev, hd, pair), F32),
            pltpu.VMEM((CORES, heads_dev, 8, pair), F32),
            pltpu.VMEM((CORES, heads_dev, 8, pair), F32),
            pltpu.VMEM((CORES, CORES, pair, half), BF16),
            pltpu.VMEM((pair, d_model), F32),
            pltpu.VMEM((pair, d_model), F32),
            pltpu.VMEM((tok, d_model), BF16),
            pltpu.VMEM((d_model, half + 2 * hd), BF16),
            pltpu.VMEM((2 * half, d_model), BF16),
            pltpu.VMEM((W_SLOTS, d_model, 2 * FF_TILE), BF16),
            pltpu.VMEM((W_SLOTS, FF_TILE, d_model), BF16),
            dma((6, 3)), dma((6, 3)), dma((n_arr,)), dma((n_arr,)), dma((n_new,)), dma((n_new,)),
            dma((12,)), dma((12,)), dma((13,)), dma((W_SLOTS, 3)),
        ],
        compiler_params=pltpu.CompilerParams(collective_id=0, has_side_effects=True, vmem_limit_bytes=67043328),
        cost_estimate=pl.CostEstimate(flops=flops, bytes_accessed=6 * d_model * ff_half, transcendentals=0),
        name="fused_blocks",
    )(x_in, *rows, *weights, *biases, *tables)


def solution(mesh):
    axis_size = mesh.shape['cp']
    rows_spec = P(('dp', 'cp'), None)
    cache_spec = P(('dp', 'cp'), None, None)
    mat_spec = P(None, None)
    vec_spec = P(None)
    layer_specs = (cache_spec, cache_spec, mat_spec, vec_spec, mat_spec, vec_spec, mat_spec, mat_spec)
    in_specs = (rows_spec,) + layer_specs + (mat_spec, mat_spec, mat_spec) + layer_specs
    out_specs = (rows_spec, rows_spec, cache_spec, cache_spec, cache_spec, cache_spec)

    def forward(x_in, cache_k1, cache_v1, w_q1, b_q1, w_k1, b_k1, w_v1, w_o1, w_gate, w_up, w_down, cache_k2, cache_v2, w_q2, b_q2, w_k2, b_k2, w_v2, w_o2):
        tok = x_in.shape[0]
        cache_dev, kv_heads, hd = cache_k1.shape
        tables = rotation_tables(axis_size, tok, cache_dev, hd)
        biases = [part.reshape(-1, hd) for part in (b_q1, b_k1, b_q2, b_k2)]
        weights = (w_q1, w_k1, w_v1, w_o1, w_gate, w_up, w_down, w_q2, w_k2, w_v2, w_o2)
        hidden, y_two, app = fused_blocks(axis_size, x_in, (cache_k1, cache_v1, cache_k2, cache_v2), weights, biases, tables)
        outs = hand_over(hidden, y_two, app)
        return (outs[0], outs[1], *(arr.reshape(tok, kv_heads, hd) for arr in outs[2:]))

    return jax.shard_map(forward, mesh=mesh, in_specs=in_specs, out_specs=out_specs, check_vma=False)
```
